256 devices in a mesh: section: 4 (over z_hi), seq: 64 (over y, z_lo, x, core).
Axes of the slice: x: 4, y: 4, z: 8 (z_hi: 4, z_lo: 2; z = z_hi * 2 + z_lo), core: 2. Of those that a mesh axis runs over, the one named last changes fastest.
Arguments:
- saved: bfloat16 [4, 3, 8192, 2304], P('section', None, 'seq'), may hold values from -16 to 16
- cotangent: bfloat16 [3, 8192, 2304], P(None, 'seq'), may hold values from -0.0390625 to 0.0390625
- slot_table: int32 [4, 3], P('section'), may hold values from 0 to 2, each once within a row
- gain: float32 [4, 2304], P('section'), may hold values from 0.25 to 1.75
- value_weight: bfloat16 [4, 2304, 1024], P('section'), may hold values from -0.125 to 0.125
- out_weight: bfloat16 [4, 2304, 1024], P('section'), may hold values from -0.1875 to 0.1875
Outputs:
- value_grad: float32 [4, 2304, 1024], P('section', 'seq')
- out_grad: float32 [4, 2304, 1024], P('section', 'seq')
- gain_grad: float32 [4, 2304], P('section')
The draws below stay inside these ranges and needn't reach their ends.
Inputs may be any that keep to these rules, and one draw needn't show every extreme that they name: `slot_table`: each row names every stash slot once.
All inputs are finite; a program needn't handle non-finite values.
Results may differ from the reference program's by a relative error of at most 0.007.
Values may be sent and summed in bfloat16 or wider, within the bound.
A program may use at most 128 MiB of HBM per device.

```python
import jax
import jax.numpy as jnp
from jax import lax

D = 2304
R = 1024
MICRO = 3
TOKENS = 8192
N_SECTION = 4


def strengthened(entries, own_key, source, target, shards_of, factor):
    owner, partner = [(jnp.arange(entries.shape[dim]) // (entries.shape[dim] // shards_of)).reshape([-1 if axis == dim else 1 for axis in range(entries.ndim)]) for dim in (source, target)]
    chosen = jax.random.permutation(own_key, shards_of)[partner]
    strong = (owner == chosen) | (owner == (partner + shards_of // 2) % shards_of)
    return jnp.where(strong, factor * entries, entries)


def block_scale(own_key, dims, pieces, low, high):
    loudness = 1.0
    for axis_at, shards_of in pieces:
        steps = jax.random.uniform(jax.random.fold_in(jax.random.fold_in(own_key, 6), axis_at), (shards_of,), jnp.float32, low / len(pieces), high / len(pieces))
        loudness = loudness * jnp.repeat(jnp.exp(steps), dims[axis_at] // shards_of).reshape((-1,) + (1,) * (len(dims) - 1 - axis_at))
    return loudness


def bell_draw(key, extent, spread, limit, shards=(), held_as=jnp.bfloat16):
    entries = spread * jax.random.normal(key, extent, jnp.float32)
    if shards:
        entries = entries * block_scale(key, extent, shards, -0.22, 0.18)
    return jnp.clip(entries, -limit, limit).astype(held_as)


def bell_draw_with(rng, extent, scale, most, shards, heavy, kind=jnp.bfloat16):
    drawn = scale * jax.random.normal(rng, extent, jnp.float32)
    if shards:
        drawn = drawn * block_scale(rng, extent, shards, -0.22, 0.18)
    return jnp.clip(strengthened(drawn, jax.random.fold_in(rng, 3), *heavy), -most, most).astype(kind)


def setup_inputs(seed: int = 0) -> dict:
    splits = jax.random.split(jax.random.key(seed), 7)
    return {
        "saved": bell_draw_with(splits[0], (N_SECTION, MICRO, TOKENS, D), 1.0, 16.0, ((0, 4), (2, 64)), (2, 3, 64, 4.0)),
        "cotangent": bell_draw(splits[1], (MICRO, TOKENS, D), ((MICRO * TOKENS) ** -0.5), 0.0390625, ((1, 64),)),
        "slot_table": jax.vmap(lambda own: jax.random.permutation(own, MICRO))(jax.random.split(splits[2], N_SECTION)).reshape((N_SECTION, MICRO)).astype(jnp.int32),
        "gain": jnp.clip(1.0 + 0.15 * jax.random.normal(splits[3], (N_SECTION, D), jnp.float32), 0.25, 1.75),
        "value_weight": bell_draw(splits[4], (N_SECTION, D, R), D ** -0.5, 0.125, ((0, 4),)),
        "out_weight": bell_draw(splits[5], (N_SECTION, D, R), R ** -0.5, 0.1875, ((0, 4),)),
    }


EPSILON = 1e-06

def normalize(inputs, gain_row):
    value_rows = inputs.astype(jnp.float32)
    inv_rms = lax.rsqrt(lax.optimization_barrier(jnp.mean(value_rows * value_rows, axis=-1, keepdims=True)) + EPSILON)
    unit_rows = value_rows * inv_rms
    return (unit_rows, inv_rms, (unit_rows * gain_row).astype(jnp.bfloat16))

def layer_backward(inputs, grad_out, gain_row, w_value, w_out):
    unit_rows, inv_rms, normed = normalize(inputs, gain_row)
    value_out = jnp.dot(normed, w_value, preferred_element_type=jnp.float32).astype(jnp.bfloat16)
    grad_value = jnp.dot(grad_out, w_out, preferred_element_type=jnp.float32).astype(jnp.bfloat16)
    grad_normed = lax.dot_general(grad_value, w_value, (((1,), (1,)), ((), ())), preferred_element_type=jnp.float32)
    gain_term = lax.optimization_barrier(jnp.sum(grad_normed * unit_rows, axis=0))
    grad_unit = grad_normed * gain_row
    grad_in = grad_out.astype(jnp.float32) + inv_rms * (grad_unit - unit_rows * lax.optimization_barrier(jnp.mean(grad_unit * unit_rows, axis=-1, keepdims=True)))
    value_term = lax.dot_general(normed, grad_value, (((0,), (0,)), ((), ())), preferred_element_type=jnp.float32)
    out_term = lax.dot_general(grad_out, value_out, (((0,), (0,)), ((), ())), preferred_element_type=jnp.float32)
    return (grad_in.astype(jnp.bfloat16), gain_term, value_term, out_term)

def reference(saved, cotangent, slot_table, gain, value_weight, out_weight):
    grads = [cotangent[micro_index] for micro_index in range(MICRO)]
    value_list = []
    out_list = []
    gain_list = []
    for section_index in reversed(range(N_SECTION)):
        value_acc = jnp.zeros((D, R), jnp.float32)
        out_acc = jnp.zeros((D, R), jnp.float32)
        gain_acc = jnp.zeros((D,), jnp.float32)
        next_grads = []
        for micro_index in range(MICRO):
            slot_index = slot_table[section_index, micro_index].astype(jnp.int32)
            inputs = lax.dynamic_index_in_dim(saved[section_index], slot_index, 0, keepdims=False)
            grad_in, gain_term, value_term, out_term = layer_backward(inputs, grads[micro_index], gain[section_index], value_weight[section_index], out_weight[section_index])
            value_acc = value_acc + value_term
            out_acc = out_acc + out_term
            gain_acc = gain_acc + gain_term
            next_grads.append(grad_in)
        grads = next_grads
        value_list.insert(0, value_acc)
        out_list.insert(0, out_acc)
        gain_list.insert(0, gain_acc)
    return (jnp.stack(value_list), jnp.stack(out_list), jnp.stack(gain_list))
```

```python
import functools

import jax
import jax.numpy as jnp
from jax import lax
from jax.experimental import pallas as pl
from jax.experimental.pallas import tpu as pltpu
from jax.sharding import PartitionSpec as P

EPSILON = 1e-06
MESH = pl.DeviceIdType.MESH
F32 = jnp.float32
BF16 = jnp.bfloat16

CHUNK = 32
NY, NZ, NX, NC = 4, 2, 4, 2
LANES = 128


def kernel(
    sections,
    slot_ref,
    gain_ref,
    x_hbm,
    cot_hbm,
    wv_hbm,
    wo_hbm,
    ov_ref,
    oo_ref,
    og_ref,
    xb,
    gb,
    wv,
    wo,
    gout,
    ll,
    rr,
    lo,
    ro,
    acc,
    gacc,
    st1,
    r1,
    st2,
    r2,
    st3,
    r3,
    fin,
    give,
    take,
    gc,
    gx,
    gy,
    gz,
    load_sem,
    g_send,
    g_recv,
    l_send,
    l_recv,
    rr_send,
    rr_recv,
    s1_send,
    s1_recv,
    s2_send,
    s2_recv,
    s3_send,
    s3_recv,
    f_send,
    f_recv,
    gc_send,
    gc_recv,
    gx_send,
    gx_recv,
    gy_send,
    gy_recv,
    gz_send,
    gz_recv,
):
    micro, tokens, width = xb.shape
    inner = wv.shape[1]
    per_micro = tokens // CHUNK
    chunks = micro * per_micro
    rows = width // (NY * NZ * NX)
    half = rows // NC

    sec = lax.axis_index("section")
    q = lax.axis_index("seq")
    core = lax.rem(q, NC)
    xi = lax.rem(q // NC, NX)
    zi = lax.rem(q // (NC * NX), NZ)
    yi = q // (NC * NX * NZ)

    def at(y, z, x, c):
        return (sec, ((y * NZ + z) * NX + x) * NC + c)

    partner = at(yi, zi, xi, 1 - core)
    x_peer = [at(yi, zi, lax.rem(xi + d, NX), core) for d in range(NX)]
    y_peer = [at(lax.rem(yi + d, NY), zi, xi, core) for d in range(NY)]
    z_peer = at(yi, 1 - zi, xi, core)
    above = (lax.rem(sec + 1, sections), q)
    below = (lax.rem(sec + sections - 1, sections), q)

    wo_load = pltpu.make_async_copy(wo_hbm, wo, load_sem.at[0])
    x_load = pltpu.make_async_copy(x_hbm, xb, load_sem.at[1])
    wv_load = pltpu.make_async_copy(wv_hbm, wv, load_sem.at[2])

    def chunk_of(k):
        return k // per_micro, pl.ds(pl.multiple_of(lax.rem(k, per_micro) * CHUNK, CHUNK), CHUNK)

    def top_load(k):
        m, at_rows = chunk_of(k)
        return pltpu.make_async_copy(cot_hbm.at[m, at_rows], gb.at[m, at_rows], g_recv.at[k])

    def down(k):
        m, at_rows = chunk_of(k)
        return pltpu.make_async_remote_copy(
            src_ref=gout.at[m, at_rows],
            dst_ref=gb.at[m, at_rows],
            send_sem=g_send.at[k],
            recv_sem=g_recv.at[k],
            device_id=below,
            device_id_type=MESH,
        )

    is_top = sec == sections - 1

    @pl.when(is_top)
    def _():
        @pl.loop(0, chunks)
        def _(k):
            top_load(k).start()

    wo_load.start()
    x_load.start()
    wv_load.start()

    barrier = pltpu.get_barrier_semaphore()
    peers = [above, below, partner, z_peer] + x_peer[1:] + y_peer[1:]
    for peer in peers:
        pl.semaphore_signal(barrier, inc=1, device_id=peer, device_id_type=MESH)
    pl.semaphore_wait(barrier, len(peers))

    wo_load.wait()
    x_load.wait()
    wv_load.wait()
    gacc[...] = jnp.zeros_like(gacc)

    def left_copy(k):
        m, at_rows = chunk_of(k)
        far = pl.ds(pl.multiple_of(tokens + lax.rem(k, per_micro) * CHUNK, CHUNK), CHUNK)
        return pltpu.make_async_remote_copy(
            src_ref=lo.at[m, at_rows],
            dst_ref=ll.at[m, far],
            send_sem=l_send.at[k],
            recv_sem=l_recv.at[k],
            device_id=partner,
            device_id_type=MESH,
        )

    def right_copy(k):
        m, at_rows = chunk_of(k)
        far = pl.ds(pl.multiple_of(tokens + lax.rem(k, per_micro) * CHUNK, CHUNK), CHUNK)
        return pltpu.make_async_remote_copy(
            src_ref=ro.at[m, at_rows],
            dst_ref=rr.at[m, far],
            send_sem=rr_send.at[k],
            recv_sem=rr_recv.at[k],
            device_id=partner,
            device_id_type=MESH,
        )

    blocks = 9
    wide = width // blocks

    def accumulate(m, first):
        @pl.loop(0, per_micro)
        def _(j):
            left_copy(m * per_micro + j).wait_recv()
            right_copy(m * per_micro + j).wait_recv()

        @pl.loop(0, blocks)
        def _(b):
            cols = pl.ds(pl.multiple_of(b * wide, wide), wide)
            term = lax.dot_general(
                ll[m, :, cols], rr[m], (((0,), (0,)), ((), ())), preferred_element_type=F32
            )
            if first:
                acc[cols, :] = term
            else:
                acc[cols, :] += term

    @pl.loop(0, chunks)
    def _(k):
        m, at_rows = chunk_of(k)

        @pl.when(is_top)
        def _():
            top_load(k).wait()

        @pl.when(jnp.logical_not(is_top))
        def _():
            down(k).wait_recv()

        g = gb[m, at_rows, :]
        slot = slot_ref[0, m]
        x = xb[slot, at_rows, :].astype(F32)
        gain = gain_ref[...]
        inv = lax.rsqrt(jnp.mean(x * x, axis=-1, keepdims=True) + EPSILON)
        unit = x * inv
        n = (unit * gain).astype(BF16)
        gv = jnp.dot(g, wo[...], preferred_element_type=F32).astype(BF16)
        gn = lax.dot_general(gv, wv[...], (((1,), (1,)), ((), ())), preferred_element_type=F32)
        gu_terms = gn * unit
        gu = gn * gain
        centre = jnp.mean(gu * unit, axis=-1, keepdims=True)
        gout[m, at_rows, :] = (g.astype(F32) + inv * (gu - unit * centre)).astype(BF16)
        part = gu_terms[0:8]
        for j in range(1, CHUNK // 8):
            part = part + gu_terms[8 * j : 8 * j + 8]
        gacc[...] += part

        @pl.when(sec > 0)
        def _():
            down(k).start()

        v = jnp.dot(n, wv[...], preferred_element_type=F32).astype(BF16)
        ll[m, at_rows, :] = jnp.where(core == 0, n, g)
        lo[m, at_rows, :] = jnp.where(core == 0, g, n)
        rr[m, at_rows, :] = jnp.where(core == 0, gv, v)
        ro[m, at_rows, :] = jnp.where(core == 0, v, gv)
        left_copy(k).start()
        right_copy(k).start()

        @pl.when(k == per_micro + 1)
        def _():
            accumulate(0, True)

        if micro > 2:

            @pl.when(jnp.logical_and(lax.rem(k, per_micro) == 1, k > 2 * per_micro))
            def _():
                accumulate(m - 1, False)

    own_gain = jnp.sum(gacc[...], axis=0, keepdims=True)
    gc[core] = own_gain
    gc_copy = pltpu.make_async_remote_copy(
        src_ref=gc.at[core],
        dst_ref=gc.at[core],
        send_sem=gc_send,
        recv_sem=gc_recv,
        device_id=partner,
        device_id_type=MESH,
    )
    gc_copy.start()

    accumulate(micro - 1, False)

    def pieces(y, z, x):
        p = (y * NZ + z) * NX + x
        return pl.ds(pl.multiple_of(p * rows, 8), rows)

    def stage_first(part, dest, hs):
        lane0 = part * 2 * LANES

        @pl.loop(0, NY * NZ)
        def _(j):
            other, z = j // NZ, lax.rem(j, NZ)
            block_rows = pieces(other, z, dest) if part == 0 else pieces(dest, z, other)
            for h in hs:
                lane = lane0 + h * LANES
                top = acc[block_rows, lane : lane + LANES]
                bottom = acc[block_rows, inner // 2 + lane : inner // 2 + lane + LANES]
                st1[part, dest, h, j] = jnp.concatenate([top, bottom], axis=0).astype(BF16)

    def ring_copy(st, r, send, recv, part, slot, src, h, peer):
        return pltpu.make_async_remote_copy(
            src_ref=st.at[part, src, h],
            dst_ref=r.at[part, slot],
            send_sem=send.at[part, slot],
            recv_sem=recv.at[part, slot],
            device_id=peer,
            device_id_type=MESH,
        )

    def ring(st, r, send, recv, part, mine, n, peer):
        plus, minus, across = lax.rem(mine + 1, n), lax.rem(mine + 3, n), lax.rem(mine + 2, n)
        to_plus, to_minus = peer[1], peer[3]
        copy = functools.partial(ring_copy, st, r, send, recv, part)
        return [
            copy(0, across, 0, to_plus),
            copy(1, across, 1, to_minus),
            copy(2, plus, 1, to_plus),
            copy(3, minus, 0, to_minus),
            copy(4, plus, 0, to_plus),
            copy(5, minus, 1, to_minus),
        ]

    dims = [(xi, NX, x_peer), (yi, NY, y_peer)]
    first = [ring(st1, r1, s1_send, s1_recv, part, *dims[part]) for part in range(2)]
    second = [ring(st2, r2, s2_send, s2_recv, part, *dims[1 - part]) for part in range(2)]

    def neighbours(i, n):
        return lax.rem(i + 1, n), lax.rem(i + 3, n), lax.rem(i + 2, n)

    for part in range(2):
        plus, minus, across = neighbours(*dims[part][:2])
        stage_first(part, across, (0, 1))
        first[part][0].start()
        first[part][1].start()
    for part in range(2):
        plus, minus, across = neighbours(*dims[part][:2])
        stage_first(part, plus, (1,))
        first[part][2].start()
        stage_first(part, minus, (0,))
        first[part][3].start()

    gc_copy.wait_recv()
    gx[xi] = gc[0] + gc[1]
    gx_copies = []
    for d in range(1, NX):
        copy = pltpu.make_async_remote_copy(
            src_ref=gx.at[xi],
            dst_ref=gx.at[xi],
            send_sem=gx_send.at[d],
            recv_sem=gx_recv.at[xi],
            device_id=x_peer[d],
            device_id_type=MESH,
        )
        copy.start()
        gx_copies.append(copy)

    for part in range(2):
        plus, minus, across = neighbours(*dims[part][:2])
        stage_first(part, plus, (0,))
        stage_first(part, minus, (1,))
        stage_first(part, dims[part][0], (0, 1))

    def hop(st, r, copies, part, mine, n, loops):
        plus, minus, across = neighbours(mine, n)
        for slot, dest, h, onward in ((0, plus, 0, 4), (1, minus, 1, 5)):
            copies[slot].wait_recv()

            @pl.loop(0, loops)
            def _(j):
                st[part, dest, h, j] = (
                    st[part, dest, h, j].astype(F32) + r[part, slot, j].astype(F32)
                ).astype(BF16)

            copies[onward].start()

    for part in range(2):
        hop(st1, r1, first[part], part, *dims[part][:2], NY * NZ)

    def gathered(buf, recv, mine, n):
        for d in range(1, n):
            j = lax.rem(mine + d, n)
            pltpu.make_async_remote_copy(
                src_ref=buf.at[j],
                dst_ref=buf.at[j],
                send_sem=gx_send.at[0],
                recv_sem=recv.at[j],
                device_id=partner,
                device_id_type=MESH,
            ).wait_recv()
        total = buf[0]
        for j in range(1, n):
            total = total + buf[j]
        return total

    gy[yi] = gathered(gx, gx_recv, xi, NX)
    gy_copies = []
    for d in range(1, NY):
        copy = pltpu.make_async_remote_copy(
            src_ref=gy.at[yi],
            dst_ref=gy.at[yi],
            send_sem=gy_send.at[d],
            recv_sem=gy_recv.at[yi],
            device_id=y_peer[d],
            device_id_type=MESH,
        )
        copy.start()
        gy_copies.append(copy)

    for part in range(2):
        mine = dims[part][0]
        for h, slots in ((0, (3, 4)), (1, (2, 5))):
            for slot in slots:
                first[part][slot].wait_recv()

            @pl.loop(0, NY * NZ)
            def _(j):
                total = (
                    st1[part, mine, h, j].astype(F32)
                    + r1[part, slots[0], j].astype(F32)
                    + r1[part, slots[1], j].astype(F32)
                )
                st2[part, j // NZ, h, lax.rem(j, NZ)] = total.astype(BF16)

        for j in range(4):
            second[part][j].start()

    gz[zi] = gathered(gy, gy_recv, yi, NY)
    gz_copy = pltpu.make_async_remote_copy(
        src_ref=gz.at[zi],
        dst_ref=gz.at[zi],
        send_sem=gz_send,
        recv_sem=gz_recv,
        device_id=z_peer,
        device_id_type=MESH,
    )
    gz_copy.start()

    for part in range(2):
        hop(st2, r2, second[part], part, *dims[1 - part][:2], NZ)

    def z_copy(part):
        return pltpu.make_async_remote_copy(
            src_ref=st3.at[part, 1 - zi],
            dst_ref=r3.at[part],
            send_sem=s3_send.at[part],
            recv_sem=s3_recv.at[part],
            device_id=z_peer,
            device_id_type=MESH,
        )

    for part in range(2):
        mine = dims[1 - part][0]
        for h, slots in ((0, (3, 4)), (1, (2, 5))):
            for slot in slots:
                second[part][slot].wait_recv()
            for z in range(NZ):
                total = (
                    st2[part, mine, h, z].astype(F32)
                    + r2[part, slots[0], z].astype(F32)
                    + r2[part, slots[1], z].astype(F32)
                )
                st3[part, z, h] = total.astype(BF16)
        z_copy(part).start()

    for part in range(2):
        z_copy(part).wait_recv()
        for h in range(2):
            total = st3[part, zi, h].astype(F32) + r3[part, h].astype(F32)
            lane = (part * 2 + h) * LANES
            fin[:, lane : lane + LANES] = total[:rows]
            fin[:, inner // 2 + lane : inner // 2 + lane + LANES] = total[rows:]

    low, high = fin[0:half, :], fin[half:rows, :]
    give[...] = jnp.where(core == 0, high, low)
    swap = pltpu.make_async_remote_copy(
        src_ref=give,
        dst_ref=take,
        send_sem=f_send,
        recv_sem=f_recv,
        device_id=partner,
        device_id_type=MESH,
    )
    swap.start()
    keep = jnp.where(core == 0, low, high)
    gz_copy.wait_recv()
    og_ref[...] = gz[0] + gz[1]
    swap.wait_recv()
    other = take[...]
    ov_ref[...] = jnp.where(core == 0, keep, other)
    oo_ref[...] = jnp.where(core == 0, other, keep)

    @pl.when(sec > 0)
    def _():
        @pl.loop(0, chunks)
        def _(k):
            down(k).wait_send()

    @pl.loop(0, chunks)
    def _(k):
        left_copy(k).wait_send()
        right_copy(k).wait_send()

    for part in range(2):
        for j in range(6):
            first[part][j].wait_send()
            second[part][j].wait_send()
        z_copy(part).wait_send()
    for copy in [gc_copy, gz_copy, swap] + gx_copies + gy_copies:
        copy.wait_send()


def per_device(sections, saved, cotangent, slot_table, gain, value_weight, out_weight):
    micro, tokens, width = cotangent.shape
    inner = value_weight.shape[2]
    rows = width // (NY * NZ * NX)
    chunks = micro * (tokens // CHUNK)
    unit = (2 * rows, LANES)
    n1 = NY * NZ
    dma = pltpu.SemaphoreType.DMA
    hbm = pl.BlockSpec(memory_space=pl.ANY)
    vmem = pl.BlockSpec(memory_space=pltpu.VMEM)
    ov, oo, og = pl.pallas_call(
        functools.partial(kernel, sections),
        out_shape=(
            jax.ShapeDtypeStruct((rows // NC, inner), F32),
            jax.ShapeDtypeStruct((rows // NC, inner), F32),
            jax.ShapeDtypeStruct((1, width), F32),
        ),
        in_specs=[pl.BlockSpec(memory_space=pltpu.SMEM), vmem, hbm, hbm, hbm, hbm],
        out_specs=(vmem, vmem, vmem),
        scratch_shapes=[
            pltpu.VMEM((micro, tokens, width), BF16),
            pltpu.VMEM((micro, tokens, width), BF16),
            pltpu.VMEM((width, inner), BF16),
            pltpu.VMEM((width, inner), BF16),
            pltpu.VMEM((micro, tokens, width), BF16),
            pltpu.VMEM((micro, 2 * tokens, width), BF16),
            pltpu.VMEM((micro, 2 * tokens, inner), BF16),
            pltpu.VMEM((micro, tokens, width), BF16),
            pltpu.VMEM((micro, tokens, inner), BF16),
            pltpu.VMEM((width, inner), F32),
            pltpu.VMEM((8, width), F32),
            pltpu.VMEM((2, 4, 2, n1) + unit, BF16),
            pltpu.VMEM((2, 6, n1) + unit, BF16),
            pltpu.VMEM((2, 4, 2, NZ) + unit, BF16),
            pltpu.VMEM((2, 6, NZ) + unit, BF16),
            pltpu.VMEM((2, NZ, 2) + unit, BF16),
            pltpu.VMEM((2, 2) + unit, BF16),
            pltpu.VMEM((rows, inner), F32),
            pltpu.VMEM((rows // NC, inner), F32),
            pltpu.VMEM((rows // NC, inner), F32),
            pltpu.VMEM((NC, 1, width), F32),
            pltpu.VMEM((NX, 1, width), F32),
            pltpu.VMEM((NY, 1, width), F32),
            pltpu.VMEM((NZ, 1, width), F32),
            dma((3,)),
            dma((chunks,)),
            dma((chunks,)),
            dma((chunks,)),
            dma((chunks,)),
            dma((chunks,)),
            dma((chunks,)),
            dma((2, 6)),
            dma((2, 6)),
            dma((2, 6)),
            dma((2, 6)),
            dma((2,)),
            dma((2,)),
            dma,
            dma,
            dma,
            dma,
            dma((NX,)),
            dma((NX,)),
            dma((NY,)),
            dma((NY,)),
            dma,
            dma,
        ],
        compiler_params=pltpu.CompilerParams(
            collective_id=0, has_side_effects=True, vmem_limit_bytes=62 * 1024 * 1024
        ),
    )(slot_table, gain, saved[0], cotangent, value_weight[0], out_weight[0])
    return (ov[None], oo[None], og)


def solution(mesh):
    in_specs = (
        P("section", None, "seq", None),
        P(None, "seq", None),
        P("section", None),
        P("section", None),
        P("section", None, None),
        P("section", None, None),
    )
    out_specs = (P("section", "seq", None), P("section", "seq", None), P("section", None))
    return jax.shard_map(
        functools.partial(per_device, mesh.shape["section"]),
        mesh=mesh,
        in_specs=in_specs,
        out_specs=out_specs,
        check_vma=False,
    )
```

```python
import functools

import jax
import jax.numpy as jnp
from jax import lax
from jax.experimental import pallas as pl
from jax.experimental.pallas import tpu as pltpu
from jax.sharding import PartitionSpec as P

EPSILON = 1e-06
MESH = pl.DeviceIdType.MESH
F32 = jnp.float32
BF16 = jnp.bfloat16

CHUNK = 32
NY, NZ, NX, NC = 4, 2, 4, 2
LANES = 128


def kernel(
    sections,
    slot_ref,
    gain_ref,
    x_hbm,
    cot_hbm,
    wv_hbm,
    wo_hbm,
    ov_ref,
    oo_ref,
    og_ref,
    xb,
    gb,
    wv,
    wo,
    wvt,
    nb,
    vb,
    gout,
    ll,
    rr,
    lo,
    ro,
    acc,
    gacc,
    st1,
    r1,
    st2,
    r2,
    st3,
    r3,
    fin,
    give,
    take,
    gc,
    gx,
    gy,
    gz,
    load_sem,
    g_send,
    g_recv,
    l_send,
    l_recv,
    rr_send,
    rr_recv,
    s1_send,
    s1_recv,
    s2_send,
    s2_recv,
    s3_send,
    s3_recv,
    f_send,
    f_recv,
    gc_send,
    gc_recv,
    gx_send,
    gx_recv,
    gy_send,
    gy_recv,
    gz_send,
    gz_recv,
):
    micro, tokens, width = xb.shape
    inner = wv.shape[1]
    per_micro = tokens // CHUNK
    chunks = micro * per_micro
    rows = width // (NY * NZ * NX)
    half = rows // NC

    sec = lax.axis_index("section")
    q = lax.axis_index("seq")
    core = lax.rem(q, NC)
    xi = lax.rem(q // NC, NX)
    zi = lax.rem(q // (NC * NX), NZ)
    yi = q // (NC * NX * NZ)

    def at(y, z, x, c):
        return (sec, ((y * NZ + z) * NX + x) * NC + c)

    partner = at(yi, zi, xi, 1 - core)
    x_peer = [at(yi, zi, lax.rem(xi + d, NX), core) for d in range(NX)]
    y_peer = [at(lax.rem(yi + d, NY), zi, xi, core) for d in range(NY)]
    z_peer = at(yi, 1 - zi, xi, core)
    above = (lax.rem(sec + 1, sections), q)
    below = (lax.rem(sec + sections - 1, sections), q)

    wo_load = pltpu.make_async_copy(wo_hbm, wo, load_sem.at[0])
    x_load = pltpu.make_async_copy(x_hbm, xb, load_sem.at[1])
    wv_load = pltpu.make_async_copy(wv_hbm, wv, load_sem.at[2])

    def chunk_of(k):
        return k // per_micro, pl.ds(pl.multiple_of(lax.rem(k, per_micro) * CHUNK, CHUNK), CHUNK)

    def top_load(k):
        m, at_rows = chunk_of(k)
        return pltpu.make_async_copy(cot_hbm.at[m, at_rows], gb.at[m, at_rows], g_recv.at[k])

    def down(k):
        m, at_rows = chunk_of(k)
        return pltpu.make_async_remote_copy(
            src_ref=gout.at[m, at_rows],
            dst_ref=gb.at[m, at_rows],
            send_sem=g_send.at[k],
            recv_sem=g_recv.at[k],
            device_id=below,
            device_id_type=MESH,
        )

    is_top = sec == sections - 1
    wv_load.start()

    @pl.when(is_top)
    def _():
        @pl.loop(0, chunks)
        def _(k):
            top_load(k).start()

    wo_load.start()
    x_load.start()

    barrier = pltpu.get_barrier_semaphore()
    peers = [above, below, partner, z_peer] + x_peer[1:] + y_peer[1:]
    for peer in peers:
        pl.semaphore_signal(barrier, inc=1, device_id=peer, device_id_type=MESH)

    gain = gain_ref[...]

    def normed(x):
        inv = lax.rsqrt(jnp.mean(x * x, axis=-1, keepdims=True) + EPSILON)
        unit = x * inv
        return inv, unit, (unit * gain).astype(BF16)

    with jax.named_scope("loads"):
        gacc[...] = jnp.zeros_like(gacc)
        wv_load.wait()

        @pl.loop(0, width // 256)
        def _(b):
            at_cols = pl.ds(pl.multiple_of(b * 256, 256), 256)
            wvt[:, at_cols] = wv[at_cols, :].T

        wo_load.wait()
        x_load.wait()

    with jax.named_scope("barrier"):
        pl.semaphore_wait(barrier, len(peers))

    with jax.named_scope("prepare"):

        @pl.when(jnp.logical_not(is_top))
        def _():
            @pl.loop(0, micro)
            def _(m):
                slot = slot_ref[0, m]

                @pl.loop(0, per_micro)
                def _(j):
                    at_rows = pl.ds(pl.multiple_of(j * CHUNK, CHUNK), CHUNK)
                    _, _, n = normed(xb[slot, at_rows, :].astype(F32))
                    nb[m, at_rows, :] = n

                vb[m] = jnp.dot(nb[m], wv[...], preferred_element_type=F32).astype(BF16)

    def left_copy(k):
        m, at_rows = chunk_of(k)
        far = pl.ds(pl.multiple_of(tokens + lax.rem(k, per_micro) * CHUNK, CHUNK), CHUNK)
        return pltpu.make_async_remote_copy(
            src_ref=lo.at[m, at_rows],
            dst_ref=ll.at[m, far],
            send_sem=l_send.at[k],
            recv_sem=l_recv.at[k],
            device_id=partner,
            device_id_type=MESH,
        )

    def right_copy(k):
        m, at_rows = chunk_of(k)
        far = pl.ds(pl.multiple_of(tokens + lax.rem(k, per_micro) * CHUNK, CHUNK), CHUNK)
        return pltpu.make_async_remote_copy(
            src_ref=ro.at[m, at_rows],
            dst_ref=rr.at[m, far],
            send_sem=rr_send.at[k],
            recv_sem=rr_recv.at[k],
            device_id=partner,
            device_id_type=MESH,
        )

    wide = 256

    def received(m):
        @pl.loop(0, per_micro)
        def _(j):
            left_copy(m * per_micro + j).wait_recv()
            right_copy(m * per_micro + j).wait_recv()

    def add_columns(m, at_cols, first):
        term = lax.dot_general(
            ll[m], rr[m, :, at_cols], (((0,), (0,)), ((), ())), preferred_element_type=F32
        )
        if first:
            acc[:, at_cols] = term
        else:
            acc[:, at_cols] += term

    def accumulate(m, first):
        received(m)

        @pl.loop(0, inner // wide)
        def _(c):
            add_columns(m, pl.ds(pl.multiple_of(c * wide, wide), wide), first)

    @pl.loop(0, chunks)
    def _(k):
        m, at_rows = chunk_of(k)

        with jax.named_scope("gwait"):

            @pl.when(is_top)
            def _():
                top_load(k).wait()

            @pl.when(jnp.logical_not(is_top))
            def _():
                down(k).wait_recv()

        with jax.named_scope("main"):
            g = gb[m, at_rows, :]
            inv, unit, n = normed(xb[slot_ref[0, m], at_rows, :].astype(F32))
            gv = jnp.dot(g, wo[...], preferred_element_type=F32).astype(BF16)
            gn = jnp.dot(gv, wvt[...], preferred_element_type=F32)
            gu_terms = gn * unit
            gu = gn * gain
            centre = jnp.mean(gu * unit, axis=-1, keepdims=True)
            gout[m, at_rows, :] = (g.astype(F32) + inv * (gu - unit * centre)).astype(BF16)
            part = gu_terms[0:8]
            for j in range(1, CHUNK // 8):
                part = part + gu_terms[8 * j : 8 * j + 8]
            gacc[...] += part

        @pl.when(sec > 0)
        def _():
            down(k).start()

        with jax.named_scope("share"):

            @pl.when(is_top)
            def _():
                vb[m, at_rows, :] = jnp.dot(n, wv[...], preferred_element_type=F32).astype(BF16)

            v = vb[m, at_rows, :]
            ll[m, at_rows, :] = jnp.where(core == 0, n, g)
            lo[m, at_rows, :] = jnp.where(core == 0, g, n)
            rr[m, at_rows, :] = jnp.where(core == 0, gv, v)
            ro[m, at_rows, :] = jnp.where(core == 0, v, gv)
            left_copy(k).start()
            right_copy(k).start()

        @pl.when(k == per_micro + 1)
        def _():
            with jax.named_scope("acc"):
                accumulate(0, True)

        if micro > 2:

            @pl.when(jnp.logical_and(lax.rem(k, per_micro) == 1, k > 2 * per_micro))
            def _():
                with jax.named_scope("acc"):
                    accumulate(m - 1, False)

    own_gain = jnp.sum(gacc[...], axis=0, keepdims=True)
    gc[core] = own_gain
    gc_copy = pltpu.make_async_remote_copy(
        src_ref=gc.at[core],
        dst_ref=gc.at[core],
        send_sem=gc_send,
        recv_sem=gc_recv,
        device_id=partner,
        device_id_type=MESH,
    )
    gc_copy.start()

    received(micro - 1)

    def pieces(y, z, x):
        p = (y * NZ + z) * NX + x
        return pl.ds(pl.multiple_of(p * rows, 8), rows)

    def stage_first(part, dest, hs):
        lane0 = part * 2 * LANES

        @pl.loop(0, NY * NZ)
        def _(j):
            other, z = j // NZ, lax.rem(j, NZ)
            block_rows = pieces(other, z, dest) if part == 0 else pieces(dest, z, other)
            for h in hs:
                lane = lane0 + h * LANES
                top = acc[block_rows, lane : lane + LANES]
                bottom = acc[block_rows, inner // 2 + lane : inner // 2 + lane + LANES]
                st1[part, dest, h, j] = jnp.concatenate([top, bottom], axis=0).astype(BF16)

    def ring_copy(st, r, send, recv, part, slot, src, h, peer):
        return pltpu.make_async_remote_copy(
            src_ref=st.at[part, src, h],
            dst_ref=r.at[part, slot],
            send_sem=send.at[part, slot],
            recv_sem=recv.at[part, slot],
            device_id=peer,
            device_id_type=MESH,
        )

    def ring(st, r, send, recv, part, mine, n, peer):
        plus, minus, across = lax.rem(mine + 1, n), lax.rem(mine + 3, n), lax.rem(mine + 2, n)
        to_plus, to_minus = peer[1], peer[3]
        copy = functools.partial(ring_copy, st, r, send, recv, part)
        return [
            copy(0, across, 0, to_plus),
            copy(1, across, 1, to_minus),
            copy(2, plus, 1, to_plus),
            copy(3, minus, 0, to_minus),
            copy(4, plus, 0, to_plus),
            copy(5, minus, 1, to_minus),
        ]

    dims = [(xi, NX, x_peer), (yi, NY, y_peer)]
    first = [ring(st1, r1, s1_send, s1_recv, part, *dims[part]) for part in range(2)]
    second = [ring(st2, r2, s2_send, s2_recv, part, *dims[1 - part]) for part in range(2)]

    def neighbours(i, n):
        return lax.rem(i + 1, n), lax.rem(i + 3, n), lax.rem(i + 2, n)

    with jax.named_scope("stage"):
        for part in range(2):
            plus, minus, across = neighbours(*dims[part][:2])
            for side in range(2):
                lane = side * (inner // 2) + part * 2 * LANES
                add_columns(micro - 1, pl.ds(lane, wide), False)
            stage_first(part, across, (0, 1))
            first[part][0].start()
            first[part][1].start()
            stage_first(part, plus, (1,))
            first[part][2].start()
            stage_first(part, minus, (0,))
            first[part][3].start()

    with jax.named_scope("gain1"):
        gc_copy.wait_recv()
        gx[xi] = gc[0] + gc[1]
        gx_copies = []
        for d in range(1, NX):
            copy = pltpu.make_async_remote_copy(
                src_ref=gx.at[xi],
                dst_ref=gx.at[xi],
                send_sem=gx_send.at[d],
                recv_sem=gx_recv.at[xi],
                device_id=x_peer[d],
                device_id_type=MESH,
            )
            copy.start()
            gx_copies.append(copy)

    with jax.named_scope("stage2"):
        for part in range(2):
            plus, minus, across = neighbours(*dims[part][:2])
            stage_first(part, plus, (0,))
            stage_first(part, minus, (1,))
            stage_first(part, dims[part][0], (0, 1))

    def hop(st, r, copies, part, mine, n, loops):
        plus, minus, across = neighbours(mine, n)
        for slot, dest, h, onward in ((0, plus, 0, 4), (1, minus, 1, 5)):
            copies[slot].wait_recv()

            @pl.loop(0, loops)
            def _(j):
                st[part, dest, h, j] = (
                    st[part, dest, h, j].astype(F32) + r[part, slot, j].astype(F32)
                ).astype(BF16)

            copies[onward].start()

    with jax.named_scope("drain1"):
        @pl.when(sec > 0)
        def _():
            @pl.loop(0, chunks)
            def _(k):
                down(k).wait_send()

        @pl.loop(0, chunks)
        def _(k):
            left_copy(k).wait_send()
            right_copy(k).wait_send()

    with jax.named_scope("hop1"):
        for part in range(2):
            hop(st1, r1, first[part], part, *dims[part][:2], NY * NZ)

    def gathered(buf, recv, mine, n):
        for d in range(1, n):
            j = lax.rem(mine + d, n)
            pltpu.make_async_remote_copy(
                src_ref=buf.at[j],
                dst_ref=buf.at[j],
                send_sem=gx_send.at[0],
                recv_sem=recv.at[j],
                device_id=partner,
                device_id_type=MESH,
            ).wait_recv()
        total = buf[0]
        for j in range(1, n):
            total = total + buf[j]
        return total

    with jax.named_scope("gain2"):
        gy[yi] = gathered(gx, gx_recv, xi, NX)
        gy_copies = []
        for d in range(1, NY):
            copy = pltpu.make_async_remote_copy(
                src_ref=gy.at[yi],
                dst_ref=gy.at[yi],
                send_sem=gy_send.at[d],
                recv_sem=gy_recv.at[yi],
                device_id=y_peer[d],
                device_id_type=MESH,
            )
            copy.start()
            gy_copies.append(copy)

    with jax.named_scope("sum1"):
        for part in range(2):
            mine = dims[part][0]
            for h, slots in ((0, (3, 4)), (1, (2, 5))):
                for slot in slots:
                    first[part][slot].wait_recv()

                @pl.loop(0, NY * NZ)
                def _(j):
                    total = (
                        st1[part, mine, h, j].astype(F32)
                        + r1[part, slots[0], j].astype(F32)
                        + r1[part, slots[1], j].astype(F32)
                    )
                    st2[part, j // NZ, h, lax.rem(j, NZ)] = total.astype(BF16)

            for j in range(4):
                second[part][j].start()

    with jax.named_scope("gain3"):
        gz[zi] = gathered(gy, gy_recv, yi, NY)
        gz_copy = pltpu.make_async_remote_copy(
            src_ref=gz.at[zi],
            dst_ref=gz.at[zi],
            send_sem=gz_send,
            recv_sem=gz_recv,
            device_id=z_peer,
            device_id_type=MESH,
        )
        gz_copy.start()

    with jax.named_scope("hop2"):
        for part in range(2):
            hop(st2, r2, second[part], part, *dims[1 - part][:2], NZ)

    def z_copy(part):
        return pltpu.make_async_remote_copy(
            src_ref=st3.at[part, 1 - zi],
            dst_ref=r3.at[part],
            send_sem=s3_send.at[part],
            recv_sem=s3_recv.at[part],
            device_id=z_peer,
            device_id_type=MESH,
        )

    with jax.named_scope("sum2"):
        for part in range(2):
            mine = dims[1 - part][0]
            for h, slots in ((0, (3, 4)), (1, (2, 5))):
                for slot in slots:
                    second[part][slot].wait_recv()
                for z in range(NZ):
                    total = (
                        st2[part, mine, h, z].astype(F32)
                        + r2[part, slots[0], z].astype(F32)
                        + r2[part, slots[1], z].astype(F32)
                    )
                    st3[part, z, h] = total.astype(BF16)
            z_copy(part).start()

    with jax.named_scope("zsum"):
        for part in range(2):
            z_copy(part).wait_recv()
            for h in range(2):
                total = st3[part, zi, h].astype(F32) + r3[part, h].astype(F32)
                lane = (part * 2 + h) * LANES
                fin[:, lane : lane + LANES] = total[:rows]
                fin[:, inner // 2 + lane : inner // 2 + lane + LANES] = total[rows:]

    with jax.named_scope("swap"):
        low, high = fin[0:half, :], fin[half:rows, :]
        give[...] = jnp.where(core == 0, high, low)
        swap = pltpu.make_async_remote_copy(
            src_ref=give,
            dst_ref=take,
            send_sem=f_send,
            recv_sem=f_recv,
            device_id=partner,
            device_id_type=MESH,
        )
        swap.start()
        keep = jnp.where(core == 0, low, high)
        gz_copy.wait_recv()
        og_ref[...] = gz[0] + gz[1]
        swap.wait_recv()
        other = take[...]
        ov_ref[...] = jnp.where(core == 0, keep, other)
        oo_ref[...] = jnp.where(core == 0, other, keep)

    with jax.named_scope("drain2"):
        for part in range(2):
            for j in range(6):
                first[part][j].wait_send()
                second[part][j].wait_send()
            z_copy(part).wait_send()
        for copy in [gc_copy, gz_copy, swap] + gx_copies + gy_copies:
            copy.wait_send()


def hand_out(ov, oo, og, ov_out, oo_out, og_out):
    ov_out[:, 0, :] = ov[...]
    oo_out[:, 0, :] = oo[...]
    og_out[...] = og[...]


def per_device(sections, saved, cotangent, slot_table, gain, value_weight, out_weight):
    micro, tokens, width = cotangent.shape
    inner = value_weight.shape[2]
    rows = width // (NY * NZ * NX)
    chunks = micro * (tokens // CHUNK)
    unit = (2 * rows, LANES)
    n1 = NY * NZ
    dma = pltpu.SemaphoreType.DMA
    hbm = pl.BlockSpec(memory_space=pl.ANY)
    vmem = pl.BlockSpec(memory_space=pltpu.VMEM)
    ov, oo, og = pl.pallas_call(
        functools.partial(kernel, sections),
        out_shape=(
            jax.ShapeDtypeStruct((rows // NC, inner), F32),
            jax.ShapeDtypeStruct((rows // NC, inner), F32),
            jax.ShapeDtypeStruct((1, width), F32),
        ),
        in_specs=[pl.BlockSpec(memory_space=pltpu.SMEM), vmem, hbm, hbm, hbm, hbm],
        out_specs=(vmem, vmem, vmem),
        scratch_shapes=[
            pltpu.VMEM((micro, tokens, width), BF16),
            pltpu.VMEM((micro, tokens, width), BF16),
            pltpu.VMEM((width, inner), BF16),
            pltpu.VMEM((width, inner), BF16),
            pltpu.VMEM((inner, width), BF16),
            pltpu.VMEM((micro, tokens, width), BF16),
            pltpu.VMEM((micro, tokens, inner), BF16),
            pltpu.VMEM((micro, tokens, width), BF16),
            pltpu.VMEM((micro, 2 * tokens, width), BF16),
            pltpu.VMEM((micro, 2 * tokens, inner), BF16),
            pltpu.VMEM((micro, tokens, width), BF16),
            pltpu.VMEM((micro, tokens, inner), BF16),
            pltpu.VMEM((width, inner), F32),
            pltpu.VMEM((8, width), F32),
            pltpu.VMEM((2, 4, 2, n1) + unit, BF16),
            pltpu.VMEM((2, 6, n1) + unit, BF16),
            pltpu.VMEM((2, 4, 2, NZ) + unit, BF16),
            pltpu.VMEM((2, 6, NZ) + unit, BF16),
            pltpu.VMEM((2, NZ, 2) + unit, BF16),
            pltpu.VMEM((2, 2) + unit, BF16),
            pltpu.VMEM((rows, inner), F32),
            pltpu.VMEM((rows // NC, inner), F32),
            pltpu.VMEM((rows // NC, inner), F32),
            pltpu.VMEM((NC, 1, width), F32),
            pltpu.VMEM((NX, 1, width), F32),
            pltpu.VMEM((NY, 1, width), F32),
            pltpu.VMEM((NZ, 1, width), F32),
            dma((3,)),
            dma((chunks,)),
            dma((chunks,)),
            dma((chunks,)),
            dma((chunks,)),
            dma((chunks,)),
            dma((chunks,)),
            dma((2, 6)),
            dma((2, 6)),
            dma((2, 6)),
            dma((2, 6)),
            dma((2,)),
            dma((2,)),
            dma,
            dma,
            dma,
            dma,
            dma((NX,)),
            dma((NX,)),
            dma((NY,)),
            dma((NY,)),
            dma,
            dma,
        ],
        compiler_params=pltpu.CompilerParams(
            collective_id=0, has_side_effects=True, vmem_limit_bytes=62 * 1024 * 1024
        ),
    )(slot_table, gain, saved[0], cotangent, value_weight[0], out_weight[0])
    ov, oo, og = pl.pallas_call(
        hand_out,
        out_shape=(
            jax.ShapeDtypeStruct((rows // NC, 1, inner), F32),
            jax.ShapeDtypeStruct((rows // NC, 1, inner), F32),
            jax.ShapeDtypeStruct((1, width), F32),
        ),
        in_specs=[vmem, vmem, vmem],
        out_specs=(vmem, vmem, vmem),
    )(ov, oo, og)
    return (jnp.transpose(ov, (1, 0, 2)), jnp.transpose(oo, (1, 0, 2)), og)


def solution(mesh):
    in_specs = (
        P("section", None, "seq", None),
        P(None, "seq", None),
        P("section", None),
        P("section", None),
        P("section", None, None),
        P("section", None, None),
    )
    out_specs = (P("section", "seq", None), P("section", "seq", None), P("section", None))
    return jax.shard_map(
        functools.partial(per_device, mesh.shape["section"]),
        mesh=mesh,
        in_specs=in_specs,
        out_specs=out_specs,
        check_vma=False,
    )
```

```python
import functools

import jax
import jax.numpy as jnp
from jax import lax
from jax.experimental import pallas as pl
from jax.experimental.pallas import tpu as pltpu
from jax.sharding import PartitionSpec as P

EPSILON = 1e-06
MESH = pl.DeviceIdType.MESH
F32 = jnp.float32
BF16 = jnp.bfloat16

CHUNK = 32
NY, NZ, NX, NC = 4, 2, 4, 2
LANES = 128


def kernel(
    sections,
    slot_ref,
    gain_ref,
    x_hbm,
    cot_hbm,
    wv_hbm,
    wo_hbm,
    ov_ref,
    oo_ref,
    og_ref,
    xb,
    gb,
    wv,
    wo,
    wvt,
    nb,
    vb,
    gout,
    ll,
    rr,
    lo,
    ro,
    acc,
    gacc,
    st1,
    r1,
    st2,
    r2,
    st3,
    r3,
    fin,
    give,
    take,
    gc,
    gx,
    gy,
    gz,
    load_sem,
    g_send,
    g_recv,
    l_send,
    l_recv,
    rr_send,
    rr_recv,
    s1_send,
    s1_recv,
    s2_send,
    s2_recv,
    s3_send,
    s3_recv,
    f_send,
    f_recv,
    gc_send,
    gc_recv,
    gx_send,
    gx_recv,
    gy_send,
    gy_recv,
    gz_send,
    gz_recv,
    turn,
):
    micro, tokens, width = xb.shape
    inner = wv.shape[1]
    per_micro = tokens // CHUNK
    chunks = micro * per_micro
    rows = width // (NY * NZ * NX)
    half = rows // NC

    sec = lax.axis_index("section")
    q = lax.axis_index("seq")
    core = lax.rem(q, NC)
    xi = lax.rem(q // NC, NX)
    zi = lax.rem(q // (NC * NX), NZ)
    yi = q // (NC * NX * NZ)

    def at(y, z, x, c):
        return (sec, ((y * NZ + z) * NX + x) * NC + c)

    partner = at(yi, zi, xi, 1 - core)
    x_peer = [at(yi, zi, lax.rem(xi + d, NX), core) for d in range(NX)]
    y_peer = [at(lax.rem(yi + d, NY), zi, xi, core) for d in range(NY)]
    z_peer = at(yi, 1 - zi, xi, core)
    above = (lax.rem(sec + 1, sections), q)
    below = (lax.rem(sec + sections - 1, sections), q)

    wo_load = pltpu.make_async_copy(wo_hbm, wo, load_sem.at[0])
    x_load = pltpu.make_async_copy(x_hbm, xb, load_sem.at[1])
    wv_load = pltpu.make_async_copy(wv_hbm, wv, load_sem.at[2])

    def chunk_of(k):
        return k // per_micro, pl.ds(pl.multiple_of(lax.rem(k, per_micro) * CHUNK, CHUNK), CHUNK)

    def top_load(k):
        m, at_rows = chunk_of(k)
        return pltpu.make_async_copy(cot_hbm.at[m, at_rows], gb.at[m, at_rows], g_recv.at[k])

    def down(k):
        m, at_rows = chunk_of(k)
        return pltpu.make_async_remote_copy(
            src_ref=gout.at[m, at_rows],
            dst_ref=gb.at[m, at_rows],
            send_sem=g_send.at[k],
            recv_sem=g_recv.at[k],
            device_id=below,
            device_id_type=MESH,
        )

    is_top = sec == sections - 1
    wv_load.start()

    @pl.when(is_top)
    def _():
        @pl.loop(0, chunks)
        def _(k):
            top_load(k).start()

    wo_load.start()
    x_load.start()

    barrier = pltpu.get_barrier_semaphore()
    peers = [above, below, partner, z_peer] + x_peer[1:] + y_peer[1:]
    for peer in peers:
        pl.semaphore_signal(barrier, inc=1, device_id=peer, device_id_type=MESH)

    gain = gain_ref[...]

    def normed(x):
        inv = lax.rsqrt(jnp.mean(x * x, axis=-1, keepdims=True) + EPSILON)
        unit = x * inv
        return inv, unit, (unit * gain).astype(BF16)

    with jax.named_scope("loads"):
        gacc[...] = jnp.zeros_like(gacc)
        wv_load.wait()

        @pl.loop(0, width // 256)
        def _(b):
            at_cols = pl.ds(pl.multiple_of(b * 256, 256), 256)
            wvt[:, at_cols] = wv[at_cols, :].T

        wo_load.wait()
        x_load.wait()

    with jax.named_scope("barrier"):
        pl.semaphore_wait(barrier, len(peers))

    with jax.named_scope("prepare"):

        @pl.when(jnp.logical_not(is_top))
        def _():
            @pl.loop(0, micro)
            def _(m):
                slot = slot_ref[0, m]

                @pl.loop(0, per_micro)
                def _(j):
                    at_rows = pl.ds(pl.multiple_of(j * CHUNK, CHUNK), CHUNK)
                    _, _, n = normed(xb[slot, at_rows, :].astype(F32))
                    nb[m, at_rows, :] = n

                vb[m] = jnp.dot(nb[m], wv[...], preferred_element_type=F32).astype(BF16)

    def left_copy(k):
        m, at_rows = chunk_of(k)
        far = pl.ds(pl.multiple_of(tokens + lax.rem(k, per_micro) * CHUNK, CHUNK), CHUNK)
        return pltpu.make_async_remote_copy(
            src_ref=lo.at[m, at_rows],
            dst_ref=ll.at[m, far],
            send_sem=l_send.at[k],
            recv_sem=l_recv.at[k],
            device_id=partner,
            device_id_type=MESH,
        )

    def right_copy(k):
        m, at_rows = chunk_of(k)
        far = pl.ds(pl.multiple_of(tokens + lax.rem(k, per_micro) * CHUNK, CHUNK), CHUNK)
        return pltpu.make_async_remote_copy(
            src_ref=ro.at[m, at_rows],
            dst_ref=rr.at[m, far],
            send_sem=rr_send.at[k],
            recv_sem=rr_recv.at[k],
            device_id=partner,
            device_id_type=MESH,
        )

    wide = 256

    def received(m):
        @pl.loop(0, per_micro)
        def _(j):
            left_copy(m * per_micro + j).wait_recv()
            right_copy(m * per_micro + j).wait_recv()

    def add_columns(m, at_cols, first):
        term = lax.dot_general(
            ll[m], rr[m, :, at_cols], (((0,), (0,)), ((), ())), preferred_element_type=F32
        )
        if first:
            acc[:, at_cols] = term
        else:
            acc[:, at_cols] += term

    def accumulate(m, first):
        received(m)

        @pl.loop(0, inner // wide)
        def _(c):
            add_columns(m, pl.ds(pl.multiple_of(c * wide, wide), wide), first)

    @pl.loop(0, chunks)
    def _(k):
        m, at_rows = chunk_of(k)

        with jax.named_scope("gwait"):

            @pl.when(is_top)
            def _():
                top_load(k).wait()

            @pl.when(jnp.logical_not(is_top))
            def _():
                down(k).wait_recv()

        with jax.named_scope("main"):
            g = gb[m, at_rows, :]
            inv, unit, n = normed(xb[slot_ref[0, m], at_rows, :].astype(F32))
            gv = jnp.dot(g, wo[...], preferred_element_type=F32).astype(BF16)
            gn = jnp.dot(gv, wvt[...], preferred_element_type=F32)
            gu_terms = gn * unit
            gu = gn * gain
            centre = jnp.mean(gu * unit, axis=-1, keepdims=True)
            gout[m, at_rows, :] = (g.astype(F32) + inv * (gu - unit * centre)).astype(BF16)
            part = gu_terms[0:8]
            for j in range(1, CHUNK // 8):
                part = part + gu_terms[8 * j : 8 * j + 8]
            gacc[...] += part

        with jax.named_scope("turn"):

            @pl.when(jnp.logical_and(is_top, k > 0))
            def _():
                @pl.when(zi == 0)
                def _():
                    down(k - 1).wait_send()
                    pl.semaphore_signal(turn, inc=1, device_id=z_peer, device_id_type=MESH)

                @pl.when(zi == 1)
                def _():
                    pl.semaphore_wait(turn, 1)

        @pl.when(sec > 0)
        def _():
            down(k).start()

        with jax.named_scope("share"):

            @pl.when(is_top)
            def _():
                vb[m, at_rows, :] = jnp.dot(n, wv[...], preferred_element_type=F32).astype(BF16)

            v = vb[m, at_rows, :]
            ll[m, at_rows, :] = jnp.where(core == 0, n, g)
            lo[m, at_rows, :] = jnp.where(core == 0, g, n)
            rr[m, at_rows, :] = jnp.where(core == 0, gv, v)
            ro[m, at_rows, :] = jnp.where(core == 0, v, gv)
            left_copy(k).start()
            right_copy(k).start()

        @pl.when(k == per_micro + 1)
        def _():
            with jax.named_scope("acc"):
                accumulate(0, True)

        if micro > 2:

            @pl.when(jnp.logical_and(lax.rem(k, per_micro) == 1, k > 2 * per_micro))
            def _():
                with jax.named_scope("acc"):
                    accumulate(m - 1, False)

    own_gain = jnp.sum(gacc[...], axis=0, keepdims=True)
    gc[core] = own_gain
    gc_copy = pltpu.make_async_remote_copy(
        src_ref=gc.at[core],
        dst_ref=gc.at[core],
        send_sem=gc_send,
        recv_sem=gc_recv,
        device_id=partner,
        device_id_type=MESH,
    )
    gc_copy.start()

    received(micro - 1)

    def pieces(y, z, x):
        p = (y * NZ + z) * NX + x
        return pl.ds(pl.multiple_of(p * rows, 8), rows)

    def stage_first(part, dest, hs):
        lane0 = part * 2 * LANES

        @pl.loop(0, NY * NZ)
        def _(j):
            other, z = j // NZ, lax.rem(j, NZ)
            block_rows = pieces(other, z, dest) if part == 0 else pieces(dest, z, other)
            for h in hs:
                lane = lane0 + h * LANES
                top = acc[block_rows, lane : lane + LANES]
                bottom = acc[block_rows, inner // 2 + lane : inner // 2 + lane + LANES]
                st1[part, dest, h, j] = jnp.concatenate([top, bottom], axis=0).astype(BF16)

    def ring_copy(st, r, send, recv, part, slot, src, h, peer):
        return pltpu.make_async_remote_copy(
            src_ref=st.at[part, src, h],
            dst_ref=r.at[part, slot],
            send_sem=send.at[part, slot],
            recv_sem=recv.at[part, slot],
            device_id=peer,
            device_id_type=MESH,
        )

    def ring(st, r, send, recv, part, mine, n, peer):
        plus, minus, across = lax.rem(mine + 1, n), lax.rem(mine + 3, n), lax.rem(mine + 2, n)
        to_plus, to_minus = peer[1], peer[3]
        copy = functools.partial(ring_copy, st, r, send, recv, part)
        return [
            copy(0, across, 0, to_plus),
            copy(1, across, 1, to_minus),
            copy(2, plus, 1, to_plus),
            copy(3, minus, 0, to_minus),
            copy(4, plus, 0, to_plus),
            copy(5, minus, 1, to_minus),
        ]

    dims = [(xi, NX, x_peer), (yi, NY, y_peer)]
    first = [ring(st1, r1, s1_send, s1_recv, part, *dims[part]) for part in range(2)]
    second = [ring(st2, r2, s2_send, s2_recv, part, *dims[1 - part]) for part in range(2)]

    def neighbours(i, n):
        return lax.rem(i + 1, n), lax.rem(i + 3, n), lax.rem(i + 2, n)

    with jax.named_scope("stage"):
        for part in range(2):
            plus, minus, across = neighbours(*dims[part][:2])
            for side in range(2):
                lane = side * (inner // 2) + part * 2 * LANES
                add_columns(micro - 1, pl.ds(lane, wide), False)
            stage_first(part, across, (0, 1))
            first[part][0].start()
            first[part][1].start()
    with jax.named_scope("gain1"):
        gc_copy.wait_recv()
        gx[xi] = gc[0] + gc[1]
        gx_copies = []
        for d in range(1, NX):
            copy = pltpu.make_async_remote_copy(
                src_ref=gx.at[xi],
                dst_ref=gx.at[xi],
                send_sem=gx_send.at[d],
                recv_sem=gx_recv.at[xi],
                device_id=x_peer[d],
                device_id_type=MESH,
            )
            copy.start()
            gx_copies.append(copy)

    with jax.named_scope("stage2"):
        for part in range(2):
            plus, minus, across = neighbours(*dims[part][:2])
            stage_first(part, plus, (1, 0))
            stage_first(part, minus, (0, 1))
            stage_first(part, dims[part][0], (0, 1))
        for part in range(2):
            for j in range(2):
                first[part][j].wait_send()
                first[part][2 + j].start()

    def hop(st, r, copies, part, mine, n, loops):
        plus, minus, across = neighbours(mine, n)
        for slot, dest, h, onward in ((0, plus, 0, 4), (1, minus, 1, 5)):
            copies[slot].wait_recv()

            @pl.loop(0, loops)
            def _(j):
                st[part, dest, h, j] = (
                    st[part, dest, h, j].astype(F32) + r[part, slot, j].astype(F32)
                ).astype(BF16)

            copies[onward].start()

    with jax.named_scope("drain1"):
        paced = jnp.logical_and(is_top, zi == 0)

        @pl.when(jnp.logical_and(sec > 0, jnp.logical_not(paced)))
        def _():
            @pl.loop(0, chunks - 1)
            def _(k):
                down(k).wait_send()

        @pl.when(sec > 0)
        def _():
            down(chunks - 1).wait_send()

        @pl.loop(0, chunks)
        def _(k):
            left_copy(k).wait_send()
            right_copy(k).wait_send()

    with jax.named_scope("hop1"):
        for part in range(2):
            hop(st1, r1, first[part], part, *dims[part][:2], NY * NZ)

    def gathered(buf, recv, mine, n):
        for d in range(1, n):
            j = lax.rem(mine + d, n)
            pltpu.make_async_remote_copy(
                src_ref=buf.at[j],
                dst_ref=buf.at[j],
                send_sem=gx_send.at[0],
                recv_sem=recv.at[j],
                device_id=partner,
                device_id_type=MESH,
            ).wait_recv()
        total = buf[0]
        for j in range(1, n):
            total = total + buf[j]
        return total

    with jax.named_scope("gain2"):
        gy[yi] = gathered(gx, gx_recv, xi, NX)
        gy_copies = []
        for d in range(1, NY):
            copy = pltpu.make_async_remote_copy(
                src_ref=gy.at[yi],
                dst_ref=gy.at[yi],
                send_sem=gy_send.at[d],
                recv_sem=gy_recv.at[yi],
                device_id=y_peer[d],
                device_id_type=MESH,
            )
            copy.start()
            gy_copies.append(copy)

    with jax.named_scope("sum1"):
        for part in range(2):
            mine = dims[part][0]
            for h, slots in ((0, (3, 4)), (1, (2, 5))):
                for slot in slots:
                    first[part][slot].wait_recv()

                @pl.loop(0, NY * NZ)
                def _(j):
                    total = (
                        st1[part, mine, h, j].astype(F32)
                        + r1[part, slots[0], j].astype(F32)
                        + r1[part, slots[1], j].astype(F32)
                    )
                    st2[part, j // NZ, h, lax.rem(j, NZ)] = total.astype(BF16)

            for j in range(4):
                second[part][j].start()

    with jax.named_scope("gain3"):
        gz[zi] = gathered(gy, gy_recv, yi, NY)
        gz_copy = pltpu.make_async_remote_copy(
            src_ref=gz.at[zi],
            dst_ref=gz.at[zi],
            send_sem=gz_send,
            recv_sem=gz_recv,
            device_id=z_peer,
            device_id_type=MESH,
        )
        gz_copy.start()

    with jax.named_scope("hop2"):
        for part in range(2):
            hop(st2, r2, second[part], part, *dims[1 - part][:2], NZ)

    def z_copy(part):
        return pltpu.make_async_remote_copy(
            src_ref=st3.at[part, 1 - zi],
            dst_ref=r3.at[part],
            send_sem=s3_send.at[part],
            recv_sem=s3_recv.at[part],
            device_id=z_peer,
            device_id_type=MESH,
        )

    with jax.named_scope("sum2"):
        for part in range(2):
            mine = dims[1 - part][0]
            for h, slots in ((0, (3, 4)), (1, (2, 5))):
                for slot in slots:
                    second[part][slot].wait_recv()
                for z in range(NZ):
                    total = (
                        st2[part, mine, h, z].astype(F32)
                        + r2[part, slots[0], z].astype(F32)
                        + r2[part, slots[1], z].astype(F32)
                    )
                    st3[part, z, h] = total.astype(BF16)
            z_copy(part).start()

    with jax.named_scope("zsum"):
        for part in range(2):
            z_copy(part).wait_recv()
            for h in range(2):
                total = st3[part, zi, h].astype(F32) + r3[part, h].astype(F32)
                lane = (part * 2 + h) * LANES
                fin[:, lane : lane + LANES] = total[:rows]
                fin[:, inner // 2 + lane : inner // 2 + lane + LANES] = total[rows:]

    with jax.named_scope("swap"):
        low, high = fin[0:half, :], fin[half:rows, :]
        give[...] = jnp.where(core == 0, high, low)
        swap = pltpu.make_async_remote_copy(
            src_ref=give,
            dst_ref=take,
            send_sem=f_send,
            recv_sem=f_recv,
            device_id=partner,
            device_id_type=MESH,
        )
        swap.start()
        keep = jnp.where(core == 0, low, high)
        gz_copy.wait_recv()
        og_ref[...] = gz[0] + gz[1]
        swap.wait_recv()
        other = take[...]
        ov_ref[...] = jnp.where(core == 0, keep, other)
        oo_ref[...] = jnp.where(core == 0, other, keep)

    with jax.named_scope("drain2"):
        for part in range(2):
            for j in range(6):
                if j > 1:
                    first[part][j].wait_send()
                second[part][j].wait_send()
            z_copy(part).wait_send()
        for copy in [gc_copy, gz_copy, swap] + gx_copies + gy_copies:
            copy.wait_send()


def hand_out(ov, oo, og, ov_out, oo_out, og_out):
    ov_out[:, 0, :] = ov[...]
    oo_out[:, 0, :] = oo[...]
    og_out[...] = og[...]


def per_device(sections, saved, cotangent, slot_table, gain, value_weight, out_weight):
    micro, tokens, width = cotangent.shape
    inner = value_weight.shape[2]
    rows = width // (NY * NZ * NX)
    chunks = micro * (tokens // CHUNK)
    unit = (2 * rows, LANES)
    n1 = NY * NZ
    dma = pltpu.SemaphoreType.DMA
    hbm = pl.BlockSpec(memory_space=pl.ANY)
    vmem = pl.BlockSpec(memory_space=pltpu.VMEM)
    ov, oo, og = pl.pallas_call(
        functools.partial(kernel, sections),
        out_shape=(
            jax.ShapeDtypeStruct((rows // NC, inner), F32),
            jax.ShapeDtypeStruct((rows // NC, inner), F32),
            jax.ShapeDtypeStruct((1, width), F32),
        ),
        in_specs=[pl.BlockSpec(memory_space=pltpu.SMEM), vmem, hbm, hbm, hbm, hbm],
        out_specs=(vmem, vmem, vmem),
        scratch_shapes=[
            pltpu.VMEM((micro, tokens, width), BF16),
            pltpu.VMEM((micro, tokens, width), BF16),
            pltpu.VMEM((width, inner), BF16),
            pltpu.VMEM((width, inner), BF16),
            pltpu.VMEM((inner, width), BF16),
            pltpu.VMEM((micro, tokens, width), BF16),
            pltpu.VMEM((micro, tokens, inner), BF16),
            pltpu.VMEM((micro, tokens, width), BF16),
            pltpu.VMEM((micro, 2 * tokens, width), BF16),
            pltpu.VMEM((micro, 2 * tokens, inner), BF16),
            pltpu.VMEM((micro, tokens, width), BF16),
            pltpu.VMEM((micro, tokens, inner), BF16),
            pltpu.VMEM((width, inner), F32),
            pltpu.VMEM((8, width), F32),
            pltpu.VMEM((2, 4, 2, n1) + unit, BF16),
            pltpu.VMEM((2, 6, n1) + unit, BF16),
            pltpu.VMEM((2, 4, 2, NZ) + unit, BF16),
            pltpu.VMEM((2, 6, NZ) + unit, BF16),
            pltpu.VMEM((2, NZ, 2) + unit, BF16),
            pltpu.VMEM((2, 2) + unit, BF16),
            pltpu.VMEM((rows, inner), F32),
            pltpu.VMEM((rows // NC, inner), F32),
            pltpu.VMEM((rows // NC, inner), F32),
            pltpu.VMEM((NC, 1, width), F32),
            pltpu.VMEM((NX, 1, width), F32),
            pltpu.VMEM((NY, 1, width), F32),
            pltpu.VMEM((NZ, 1, width), F32),
            dma((3,)),
            dma((chunks,)),
            dma((chunks,)),
            dma((chunks,)),
            dma((chunks,)),
            dma((chunks,)),
            dma((chunks,)),
            dma((2, 6)),
            dma((2, 6)),
            dma((2, 6)),
            dma((2, 6)),
            dma((2,)),
            dma((2,)),
            dma,
            dma,
            dma,
            dma,
            dma((NX,)),
            dma((NX,)),
            dma((NY,)),
            dma((NY,)),
            dma,
            dma,
            pltpu.SemaphoreType.REGULAR,
        ],
        compiler_params=pltpu.CompilerParams(
            collective_id=0, has_side_effects=True, vmem_limit_bytes=62 * 1024 * 1024
        ),
    )(slot_table, gain, saved[0], cotangent, value_weight[0], out_weight[0])
    ov, oo, og = pl.pallas_call(
        hand_out,
        out_shape=(
            jax.ShapeDtypeStruct((rows // NC, 1, inner), F32),
            jax.ShapeDtypeStruct((rows // NC, 1, inner), F32),
            jax.ShapeDtypeStruct((1, width), F32),
        ),
        in_specs=[vmem, vmem, vmem],
        out_specs=(vmem, vmem, vmem),
    )(ov, oo, og)
    return (jnp.transpose(ov, (1, 0, 2)), jnp.transpose(oo, (1, 0, 2)), og)


def solution(mesh):
    in_specs = (
        P("section", None, "seq", None),
        P(None, "seq", None),
        P("section", None),
        P("section", None),
        P("section", None, None),
        P("section", None, None),
    )
    out_specs = (P("section", "seq", None), P("section", "seq", None), P("section", None))
    return jax.shard_map(
        functools.partial(per_device, mesh.shape["section"]),
        mesh=mesh,
        in_specs=in_specs,
        out_specs=out_specs,
        check_vma=False,
    )
```

```python
import functools

import jax
import jax.numpy as jnp
from jax import lax
from jax.experimental import pallas as pl
from jax.experimental.pallas import tpu as pltpu
from jax.sharding import PartitionSpec as P

EPSILON = 1e-06
MESH = pl.DeviceIdType.MESH
F32 = jnp.float32
BF16 = jnp.bfloat16

CHUNK = 32
NY, NZ, NX, NC = 4, 2, 4, 2
LANES = 128


def kernel(
    sections,
    slot_ref,
    gain_ref,
    x_hbm,
    cot_hbm,
    wv_hbm,
    wo_hbm,
    ov_ref,
    oo_ref,
    og_ref,
    xb,
    gb,
    wv,
    wo,
    wvt,
    nb,
    vb,
    gout,
    ll,
    rr,
    lo,
    ro,
    acc,
    gacc,
    st1,
    r1,
    st2,
    r2,
    st3,
    r3,
    fin,
    give,
    take,
    gc,
    gx,
    gy,
    gz,
    load_sem,
    g_send,
    g_recv,
    l_send,
    l_recv,
    rr_send,
    rr_recv,
    s1_send,
    s1_recv,
    s2_send,
    s2_recv,
    s3_send,
    s3_recv,
    f_send,
    f_recv,
    gc_send,
    gc_recv,
    gx_send,
    gx_recv,
    gy_send,
    gy_recv,
    gz_send,
    gz_recv,
    turn,
    ub,
    u_recv,
    u_send,
):
    micro, tokens, width = xb.shape
    inner = wv.shape[1]
    per_micro = tokens // CHUNK
    chunks = micro * per_micro
    rows = width // (NY * NZ * NX)
    half = rows // NC
    ups = chunks // 4
    downs = chunks - ups

    sec = lax.axis_index("section")
    q = lax.axis_index("seq")
    core = lax.rem(q, NC)
    xi = lax.rem(q // NC, NX)
    zi = lax.rem(q // (NC * NX), NZ)
    yi = q // (NC * NX * NZ)

    def at(y, z, x, c):
        return (sec, ((y * NZ + z) * NX + x) * NC + c)

    partner = at(yi, zi, xi, 1 - core)
    x_peer = [at(yi, zi, lax.rem(xi + d, NX), core) for d in range(NX)]
    y_peer = [at(lax.rem(yi + d, NY), zi, xi, core) for d in range(NY)]
    z_peer = at(yi, 1 - zi, xi, core)
    above = (lax.rem(sec + 1, sections), q)
    below = (lax.rem(sec + sections - 1, sections), q)

    def along_z(steps):
        z = lax.rem(sec * NZ + zi + steps, sections * NZ)
        return (z // NZ, ((yi * NZ + lax.rem(z, NZ)) * NX + xi) * NC + core)

    up_far, down_far = along_z(3), along_z(sections * NZ - 3)

    wo_load = pltpu.make_async_copy(wo_hbm, wo, load_sem.at[0])
    x_load = pltpu.make_async_copy(x_hbm, xb, load_sem.at[1])
    wv_load = pltpu.make_async_copy(wv_hbm, wv, load_sem.at[2])

    def chunk_of(k):
        return k // per_micro, pl.ds(pl.multiple_of(lax.rem(k, per_micro) * CHUNK, CHUNK), CHUNK)

    def top_load(k):
        m, at_rows = chunk_of(k)
        return pltpu.make_async_copy(cot_hbm.at[m, at_rows], gb.at[m, at_rows], g_recv.at[k])

    def down(k):
        m, at_rows = chunk_of(k)
        return pltpu.make_async_remote_copy(
            src_ref=gout.at[m, at_rows],
            dst_ref=gb.at[m, at_rows],
            send_sem=g_send.at[k],
            recv_sem=g_recv.at[k],
            device_id=below,
            device_id_type=MESH,
        )

    def up(n):
        m, at_rows = chunk_of(downs + n)
        return pltpu.make_async_remote_copy(
            src_ref=gout.at[m, at_rows],
            dst_ref=ub.at[n],
            send_sem=g_send.at[downs + n],
            recv_sem=u_recv.at[n],
            device_id=up_far,
            device_id_type=MESH,
        )

    def onward(n):
        m, at_rows = chunk_of(downs + n)
        return pltpu.make_async_remote_copy(
            src_ref=ub.at[n],
            dst_ref=gb.at[m, at_rows],
            send_sem=u_send.at[n],
            recv_sem=g_recv.at[downs + n],
            device_id=up_far,
            device_id_type=MESH,
        )

    def relay(n):
        with jax.named_scope("relay"):
            up(n).wait_recv()
            onward(n).start()

    never = 4 * chunks
    relay_odd = jnp.where(sec == 0, -ups, jnp.where(sec == 2, 8, jnp.where(sec == 3, 7, never)))
    relay_even = jnp.where(sec == 0, 0, jnp.where(sec == 1, -1, jnp.where(sec == 3, 9, never)))
    relay_at = jnp.where(zi == 1, relay_odd, relay_even)
    lead = sections - sec

    def order(i):
        j = i - lead
        mixed = jnp.where(lax.rem(j, 2) == 0, downs + j // 2, lead + (j - 1) // 2)
        late = jnp.where(j < 2 * ups - 1, mixed, i - ups)
        return jnp.where(i < lead, i, late)

    is_top = sec == sections - 1
    wv_load.start()

    @pl.when(is_top)
    def _():
        @pl.loop(0, chunks)
        def _(k):
            top_load(k).start()

    wo_load.start()
    x_load.start()

    barrier = pltpu.get_barrier_semaphore()
    peers = [above, below, up_far, down_far, partner, z_peer] + x_peer[1:] + y_peer[1:]
    for peer in peers:
        pl.semaphore_signal(barrier, inc=1, device_id=peer, device_id_type=MESH)

    gain = gain_ref[...]

    def normed(x):
        inv = lax.rsqrt(jnp.mean(x * x, axis=-1, keepdims=True) + EPSILON)
        unit = x * inv
        return inv, unit, (unit * gain).astype(BF16)

    with jax.named_scope("loads"):
        gacc[...] = jnp.zeros_like(gacc)
        wv_load.wait()

        @pl.loop(0, width // 256)
        def _(b):
            at_cols = pl.ds(pl.multiple_of(b * 256, 256), 256)
            wvt[:, at_cols] = wv[at_cols, :].T

        wo_load.wait()
        x_load.wait()

    with jax.named_scope("barrier"):
        pl.semaphore_wait(barrier, len(peers))

    with jax.named_scope("prepare"):

        @pl.when(jnp.logical_not(is_top))
        def _():
            @pl.loop(0, micro)
            def _(m):
                slot = slot_ref[0, m]

                @pl.loop(0, per_micro)
                def _(j):
                    at_rows = pl.ds(pl.multiple_of(j * CHUNK, CHUNK), CHUNK)
                    _, _, n = normed(xb[slot, at_rows, :].astype(F32))
                    nb[m, at_rows, :] = n

                vb[m] = jnp.dot(nb[m], wv[...], preferred_element_type=F32).astype(BF16)

    def left_copy(k):
        m, at_rows = chunk_of(k)
        far = pl.ds(pl.multiple_of(tokens + lax.rem(k, per_micro) * CHUNK, CHUNK), CHUNK)
        return pltpu.make_async_remote_copy(
            src_ref=lo.at[m, at_rows],
            dst_ref=ll.at[m, far],
            send_sem=l_send.at[k],
            recv_sem=l_recv.at[k],
            device_id=partner,
            device_id_type=MESH,
        )

    def right_copy(k):
        m, at_rows = chunk_of(k)
        far = pl.ds(pl.multiple_of(tokens + lax.rem(k, per_micro) * CHUNK, CHUNK), CHUNK)
        return pltpu.make_async_remote_copy(
            src_ref=ro.at[m, at_rows],
            dst_ref=rr.at[m, far],
            send_sem=rr_send.at[k],
            recv_sem=rr_recv.at[k],
            device_id=partner,
            device_id_type=MESH,
        )

    wide = 256

    def received(m):
        @pl.loop(0, per_micro)
        def _(j):
            left_copy(m * per_micro + j).wait_recv()
            right_copy(m * per_micro + j).wait_recv()

    def add_columns(m, at_cols, first):
        term = lax.dot_general(
            ll[m], rr[m, :, at_cols], (((0,), (0,)), ((), ())), preferred_element_type=F32
        )
        if first:
            acc[:, at_cols] = term
        else:
            acc[:, at_cols] += term

    def accumulate(m, first):
        received(m)

        @pl.loop(0, inner // wide)
        def _(c):
            add_columns(m, pl.ds(pl.multiple_of(c * wide, wide), wide), first)

    @pl.loop(0, ups)
    def _(n):
        @pl.when(n < -relay_at)
        def _():
            relay(n)

    @pl.loop(0, chunks)
    def _(i):
        k = order(i)
        m, at_rows = chunk_of(k)
        pm, p_rows = chunk_of(i)

        with jax.named_scope("gwait"):

            @pl.when(is_top)
            def _():
                top_load(k).wait()

            @pl.when(jnp.logical_not(is_top))
            def _():
                down(k).wait_recv()

        with jax.named_scope("main"):
            g = gb[m, at_rows, :]
            inv, unit, n = normed(xb[slot_ref[0, m], at_rows, :].astype(F32))
            gv = jnp.dot(g, wo[...], preferred_element_type=F32).astype(BF16)
            gn = jnp.dot(gv, wvt[...], preferred_element_type=F32)
            gu_terms = gn * unit
            gu = gn * gain
            centre = jnp.mean(gu * unit, axis=-1, keepdims=True)
            gout[m, at_rows, :] = (g.astype(F32) + inv * (gu - unit * centre)).astype(BF16)
            part = gu_terms[0:8]
            for j in range(1, CHUNK // 8):
                part = part + gu_terms[8 * j : 8 * j + 8]
            gacc[...] += part

        with jax.named_scope("turn"):

            @pl.when(jnp.logical_and(is_top, jnp.logical_and(k > 0, k < downs)))
            def _():
                @pl.when(zi == 0)
                def _():
                    down(k - 1).wait_send()
                    pl.semaphore_signal(turn, inc=1, device_id=z_peer, device_id_type=MESH)

                @pl.when(zi == 1)
                def _():
                    pl.semaphore_wait(turn, 1)

        @pl.when(jnp.logical_and(sec > 0, k < downs))
        def _():
            down(k).start()

        @pl.when(jnp.logical_and(sec > 0, k >= downs))
        def _():
            up(k - downs).start()

        with jax.named_scope("share"):

            @pl.when(is_top)
            def _():
                vb[m, at_rows, :] = jnp.dot(n, wv[...], preferred_element_type=F32).astype(BF16)

            v = vb[m, at_rows, :]
            ll[pm, p_rows, :] = jnp.where(core == 0, n, g)
            lo[pm, p_rows, :] = jnp.where(core == 0, g, n)
            rr[pm, p_rows, :] = jnp.where(core == 0, gv, v)
            ro[pm, p_rows, :] = jnp.where(core == 0, v, gv)
            left_copy(i).start()
            right_copy(i).start()

        @pl.when(jnp.logical_and(i >= relay_at, i < relay_at + ups))
        def _():
            relay(i - relay_at)

        @pl.when(i == per_micro + 1)
        def _():
            with jax.named_scope("acc"):
                accumulate(0, True)

        if micro > 2:

            @pl.when(jnp.logical_and(lax.rem(i, per_micro) == 1, i > 2 * per_micro))
            def _():
                with jax.named_scope("acc"):
                    accumulate(pm - 1, False)

    own_gain = jnp.sum(gacc[...], axis=0, keepdims=True)
    gc[core] = own_gain
    gc_copy = pltpu.make_async_remote_copy(
        src_ref=gc.at[core],
        dst_ref=gc.at[core],
        send_sem=gc_send,
        recv_sem=gc_recv,
        device_id=partner,
        device_id_type=MESH,
    )
    gc_copy.start()

    received(micro - 1)

    def pieces(y, z, x):
        p = (y * NZ + z) * NX + x
        return pl.ds(pl.multiple_of(p * rows, 8), rows)

    def stage_first(part, dest, hs):
        lane0 = part * 2 * LANES

        @pl.loop(0, NY * NZ)
        def _(j):
            other, z = j // NZ, lax.rem(j, NZ)
            block_rows = pieces(other, z, dest) if part == 0 else pieces(dest, z, other)
            for h in hs:
                lane = lane0 + h * LANES
                top = acc[block_rows, lane : lane + LANES]
                bottom = acc[block_rows, inner // 2 + lane : inner // 2 + lane + LANES]
                st1[part, dest, h, j] = jnp.concatenate([top, bottom], axis=0).astype(BF16)

    def ring_copy(st, r, send, recv, part, slot, src, h, peer):
        return pltpu.make_async_remote_copy(
            src_ref=st.at[part, src, h],
            dst_ref=r.at[part, slot],
            send_sem=send.at[part, slot],
            recv_sem=recv.at[part, slot],
            device_id=peer,
            device_id_type=MESH,
        )

    def ring(st, r, send, recv, part, mine, n, peer):
        plus, minus, across = lax.rem(mine + 1, n), lax.rem(mine + 3, n), lax.rem(mine + 2, n)
        to_plus, to_minus = peer[1], peer[3]
        copy = functools.partial(ring_copy, st, r, send, recv, part)
        return [
            copy(0, across, 0, to_plus),
            copy(1, across, 1, to_minus),
            copy(2, plus, 1, to_plus),
            copy(3, minus, 0, to_minus),
            copy(4, plus, 0, to_plus),
            copy(5, minus, 1, to_minus),
        ]

    dims = [(xi, NX, x_peer), (yi, NY, y_peer)]
    first = [ring(st1, r1, s1_send, s1_recv, part, *dims[part]) for part in range(2)]
    second = [ring(st2, r2, s2_send, s2_recv, part, *dims[1 - part]) for part in range(2)]

    def neighbours(i, n):
        return lax.rem(i + 1, n), lax.rem(i + 3, n), lax.rem(i + 2, n)

    with jax.named_scope("stage"):
        for part in range(2):
            plus, minus, across = neighbours(*dims[part][:2])
            for side in range(2):
                lane = side * (inner // 2) + part * 2 * LANES
                add_columns(micro - 1, pl.ds(lane, wide), False)
            stage_first(part, across, (0, 1))
            first[part][0].start()
            first[part][1].start()
    with jax.named_scope("gain1"):
        gc_copy.wait_recv()
        gx[xi] = gc[0] + gc[1]
        gx_copies = []
        for d in range(1, NX):
            copy = pltpu.make_async_remote_copy(
                src_ref=gx.at[xi],
                dst_ref=gx.at[xi],
                send_sem=gx_send.at[d],
                recv_sem=gx_recv.at[xi],
                device_id=x_peer[d],
                device_id_type=MESH,
            )
            copy.start()
            gx_copies.append(copy)

    with jax.named_scope("stage2"):
        for part in range(2):
            plus, minus, across = neighbours(*dims[part][:2])
            stage_first(part, plus, (1, 0))
            stage_first(part, minus, (0, 1))
            stage_first(part, dims[part][0], (0, 1))
        for part in range(2):
            for j in range(2):
                first[part][j].wait_send()
                first[part][2 + j].start()

    def hop(st, r, copies, part, mine, n, loops):
        plus, minus, across = neighbours(mine, n)
        for slot, dest, h, onward in ((0, plus, 0, 4), (1, minus, 1, 5)):
            copies[slot].wait_recv()

            @pl.loop(0, loops)
            def _(j):
                st[part, dest, h, j] = (
                    st[part, dest, h, j].astype(F32) + r[part, slot, j].astype(F32)
                ).astype(BF16)

            copies[onward].start()

    with jax.named_scope("drain1"):
        paced = jnp.logical_and(is_top, zi == 0)

        @pl.when(jnp.logical_and(sec > 0, jnp.logical_not(paced)))
        def _():
            @pl.loop(0, downs - 1)
            def _(k):
                down(k).wait_send()

        @pl.when(sec > 0)
        def _():
            down(downs - 1).wait_send()

            @pl.loop(0, ups)
            def _(n):
                up(n).wait_send()

        @pl.when(relay_at < never)
        def _():
            @pl.loop(0, ups)
            def _(n):
                onward(n).wait_send()

        @pl.loop(0, chunks)
        def _(k):
            left_copy(k).wait_send()
            right_copy(k).wait_send()

    with jax.named_scope("hop1"):
        for part in range(2):
            hop(st1, r1, first[part], part, *dims[part][:2], NY * NZ)

    def gathered(buf, recv, mine, n):
        for d in range(1, n):
            j = lax.rem(mine + d, n)
            pltpu.make_async_remote_copy(
                src_ref=buf.at[j],
                dst_ref=buf.at[j],
                send_sem=gx_send.at[0],
                recv_sem=recv.at[j],
                device_id=partner,
                device_id_type=MESH,
            ).wait_recv()
        total = buf[0]
        for j in range(1, n):
            total = total + buf[j]
        return total

    with jax.named_scope("gain2"):
        gy[yi] = gathered(gx, gx_recv, xi, NX)
        gy_copies = []
        for d in range(1, NY):
            copy = pltpu.make_async_remote_copy(
                src_ref=gy.at[yi],
                dst_ref=gy.at[yi],
                send_sem=gy_send.at[d],
                recv_sem=gy_recv.at[yi],
                device_id=y_peer[d],
                device_id_type=MESH,
            )
            copy.start()
            gy_copies.append(copy)

    with jax.named_scope("sum1"):
        for part in range(2):
            mine = dims[part][0]
            for h, slots in ((0, (3, 4)), (1, (2, 5))):
                for slot in slots:
                    first[part][slot].wait_recv()

                @pl.loop(0, NY * NZ)
                def _(j):
                    total = (
                        st1[part, mine, h, j].astype(F32)
                        + r1[part, slots[0], j].astype(F32)
                        + r1[part, slots[1], j].astype(F32)
                    )
                    st2[part, j // NZ, h, lax.rem(j, NZ)] = total.astype(BF16)

            for j in range(4):
                second[part][j].start()

    with jax.named_scope("gain3"):
        gz[zi] = gathered(gy, gy_recv, yi, NY)
        gz_copy = pltpu.make_async_remote_copy(
            src_ref=gz.at[zi],
            dst_ref=gz.at[zi],
            send_sem=gz_send,
            recv_sem=gz_recv,
            device_id=z_peer,
            device_id_type=MESH,
        )
        gz_copy.start()

    with jax.named_scope("hop2"):
        for part in range(2):
            hop(st2, r2, second[part], part, *dims[1 - part][:2], NZ)

    def z_copy(part):
        return pltpu.make_async_remote_copy(
            src_ref=st3.at[part, 1 - zi],
            dst_ref=r3.at[part],
            send_sem=s3_send.at[part],
            recv_sem=s3_recv.at[part],
            device_id=z_peer,
            device_id_type=MESH,
        )

    with jax.named_scope("sum2"):
        for part in range(2):
            mine = dims[1 - part][0]
            for h, slots in ((0, (3, 4)), (1, (2, 5))):
                for slot in slots:
                    second[part][slot].wait_recv()
                for z in range(NZ):
                    total = (
                        st2[part, mine, h, z].astype(F32)
                        + r2[part, slots[0], z].astype(F32)
                        + r2[part, slots[1], z].astype(F32)
                    )
                    st3[part, z, h] = total.astype(BF16)
            z_copy(part).start()

    with jax.named_scope("zsum"):
        for part in range(2):
            z_copy(part).wait_recv()
            for h in range(2):
                total = st3[part, zi, h].astype(F32) + r3[part, h].astype(F32)
                lane = (part * 2 + h) * LANES
                fin[:, lane : lane + LANES] = total[:rows]
                fin[:, inner // 2 + lane : inner // 2 + lane + LANES] = total[rows:]

    with jax.named_scope("swap"):
        low, high = fin[0:half, :], fin[half:rows, :]
        give[...] = jnp.where(core == 0, high, low)
        swap = pltpu.make_async_remote_copy(
            src_ref=give,
            dst_ref=take,
            send_sem=f_send,
            recv_sem=f_recv,
            device_id=partner,
            device_id_type=MESH,
        )
        swap.start()
        keep = jnp.where(core == 0, low, high)
        gz_copy.wait_recv()
        og_ref[...] = gz[0] + gz[1]
        swap.wait_recv()
        other = take[...]
        ov_ref[...] = jnp.where(core == 0, keep, other)
        oo_ref[...] = jnp.where(core == 0, other, keep)

    with jax.named_scope("drain2"):
        for part in range(2):
            for j in range(6):
                if j > 1:
                    first[part][j].wait_send()
                second[part][j].wait_send()
            z_copy(part).wait_send()
        for copy in [gc_copy, gz_copy, swap] + gx_copies + gy_copies:
            copy.wait_send()


def hand_out(ov, oo, og, ov_out, oo_out, og_out):
    ov_out[:, 0, :] = ov[...]
    oo_out[:, 0, :] = oo[...]
    og_out[...] = og[...]


def per_device(sections, saved, cotangent, slot_table, gain, value_weight, out_weight):
    micro, tokens, width = cotangent.shape
    inner = value_weight.shape[2]
    rows = width // (NY * NZ * NX)
    chunks = micro * (tokens // CHUNK)
    unit = (2 * rows, LANES)
    n1 = NY * NZ
    dma = pltpu.SemaphoreType.DMA
    hbm = pl.BlockSpec(memory_space=pl.ANY)
    vmem = pl.BlockSpec(memory_space=pltpu.VMEM)
    ov, oo, og = pl.pallas_call(
        functools.partial(kernel, sections),
        out_shape=(
            jax.ShapeDtypeStruct((rows // NC, inner), F32),
            jax.ShapeDtypeStruct((rows // NC, inner), F32),
            jax.ShapeDtypeStruct((1, width), F32),
        ),
        in_specs=[pl.BlockSpec(memory_space=pltpu.SMEM), vmem, hbm, hbm, hbm, hbm],
        out_specs=(vmem, vmem, vmem),
        scratch_shapes=[
            pltpu.VMEM((micro, tokens, width), BF16),
            pltpu.VMEM((micro, tokens, width), BF16),
            pltpu.VMEM((width, inner), BF16),
            pltpu.VMEM((width, inner), BF16),
            pltpu.VMEM((inner, width), BF16),
            pltpu.VMEM((micro, tokens, width), BF16),
            pltpu.VMEM((micro, tokens, inner), BF16),
            pltpu.VMEM((micro, tokens, width), BF16),
            pltpu.VMEM((micro, 2 * tokens, width), BF16),
            pltpu.VMEM((micro, 2 * tokens, inner), BF16),
            pltpu.VMEM((micro, tokens, width), BF16),
            pltpu.VMEM((micro, tokens, inner), BF16),
            pltpu.VMEM((width, inner), F32),
            pltpu.VMEM((8, width), F32),
            pltpu.VMEM((2, 4, 2, n1) + unit, BF16),
            pltpu.VMEM((2, 6, n1) + unit, BF16),
            pltpu.VMEM((2, 4, 2, NZ) + unit, BF16),
            pltpu.VMEM((2, 6, NZ) + unit, BF16),
            pltpu.VMEM((2, NZ, 2) + unit, BF16),
            pltpu.VMEM((2, 2) + unit, BF16),
            pltpu.VMEM((rows, inner), F32),
            pltpu.VMEM((rows // NC, inner), F32),
            pltpu.VMEM((rows // NC, inner), F32),
            pltpu.VMEM((NC, 1, width), F32),
            pltpu.VMEM((NX, 1, width), F32),
            pltpu.VMEM((NY, 1, width), F32),
            pltpu.VMEM((NZ, 1, width), F32),
            dma((3,)),
            dma((chunks,)),
            dma((chunks,)),
            dma((chunks,)),
            dma((chunks,)),
            dma((chunks,)),
            dma((chunks,)),
            dma((2, 6)),
            dma((2, 6)),
            dma((2, 6)),
            dma((2, 6)),
            dma((2,)),
            dma((2,)),
            dma,
            dma,
            dma,
            dma,
            dma((NX,)),
            dma((NX,)),
            dma((NY,)),
            dma((NY,)),
            dma,
            dma,
            pltpu.SemaphoreType.REGULAR,
            pltpu.VMEM((chunks // 4, CHUNK, width), BF16),
            dma((chunks // 4,)),
            dma((chunks // 4,)),
        ],
        compiler_params=pltpu.CompilerParams(
            collective_id=0, has_side_effects=True, vmem_limit_bytes=62 * 1024 * 1024
        ),
    )(slot_table, gain, saved[0], cotangent, value_weight[0], out_weight[0])
    ov, oo, og = pl.pallas_call(
        hand_out,
        out_shape=(
            jax.ShapeDtypeStruct((rows // NC, 1, inner), F32),
            jax.ShapeDtypeStruct((rows // NC, 1, inner), F32),
            jax.ShapeDtypeStruct((1, width), F32),
        ),
        in_specs=[vmem, vmem, vmem],
        out_specs=(vmem, vmem, vmem),
    )(ov, oo, og)
    return (jnp.transpose(ov, (1, 0, 2)), jnp.transpose(oo, (1, 0, 2)), og)


def solution(mesh):
    in_specs = (
        P("section", None, "seq", None),
        P(None, "seq", None),
        P("section", None),
        P("section", None),
        P("section", None, None),
        P("section", None, None),
    )
    out_specs = (P("section", "seq", None), P("section", "seq", None), P("section", None))
    return jax.shard_map(
        functools.partial(per_device, mesh.shape["section"]),
        mesh=mesh,
        in_specs=in_specs,
        out_specs=out_specs,
        check_vma=False,
    )
```

```python
import functools

import jax
import jax.numpy as jnp
from jax import lax
from jax.experimental import pallas as pl
from jax.experimental.pallas import tpu as pltpu
from jax.sharding import PartitionSpec as P

EPSILON = 1e-06
MESH = pl.DeviceIdType.MESH
F32 = jnp.float32
BF16 = jnp.bfloat16

CHUNK = 32
NY, NZ, NX, NC = 4, 2, 4, 2
LANES = 128
HALF_ROWS = 112
PAIR_ROWS = 32


def kernel(
    sections,
    slot_ref,
    gain_ref,
    x_hbm,
    cot_hbm,
    wv_hbm,
    wo_hbm,
    ov_ref,
    oo_ref,
    og_ref,
    xb,
    gb,
    wv,
    wo,
    wvt,
    nb,
    vb,
    gout,
    ll,
    rr,
    lo,
    ro,
    acc,
    gacc,
    st1,
    r1,
    st2,
    r2,
    st3,
    r3,
    stc,
    rc,
    st4,
    r4,
    st5,
    r5,
    fin,
    give,
    take,
    gc,
    gx,
    gy,
    gz,
    load_sem,
    g_send,
    g_recv,
    l_send,
    l_recv,
    rr_send,
    rr_recv,
    s1_send,
    s1_recv,
    s2_send,
    s2_recv,
    s3_send,
    s3_recv,
    sc_send,
    sc_recv,
    s4_send,
    s4_recv,
    s5_send,
    s5_recv,
    f_send,
    f_recv,
    gc_send,
    gc_recv,
    gx_send,
    gx_recv,
    gy_send,
    gy_recv,
    gz_send,
    gz_recv,
    turn,
    ub,
    u_recv,
    u_send,
):
    micro, tokens, width = xb.shape
    inner = wv.shape[1]
    per_micro = tokens // CHUNK
    chunks = micro * per_micro
    rows = width // (NY * NZ * NX)
    half = rows // NC
    ups = chunks // 4
    downs = chunks - ups

    sec = lax.axis_index("section")
    q = lax.axis_index("seq")
    core = lax.rem(q, NC)
    xi = lax.rem(q // NC, NX)
    zi = lax.rem(q // (NC * NX), NZ)
    yi = q // (NC * NX * NZ)

    def at(y, z, x, c):
        return (sec, ((y * NZ + z) * NX + x) * NC + c)

    partner = at(yi, zi, xi, 1 - core)
    x_peer = [at(yi, zi, lax.rem(xi + d, NX), core) for d in range(NX)]
    y_peer = [at(lax.rem(yi + d, NY), zi, xi, core) for d in range(NY)]
    z_peer = at(yi, 1 - zi, xi, core)
    above = (lax.rem(sec + 1, sections), q)
    below = (lax.rem(sec + sections - 1, sections), q)

    def along_z(steps):
        z = lax.rem(sec * NZ + zi + steps, sections * NZ)
        return (z // NZ, ((yi * NZ + lax.rem(z, NZ)) * NX + xi) * NC + core)

    up_far, down_far = along_z(3), along_z(sections * NZ - 3)

    wo_load = pltpu.make_async_copy(wo_hbm, wo, load_sem.at[0])
    x_load = pltpu.make_async_copy(x_hbm, xb, load_sem.at[1])
    wv_load = pltpu.make_async_copy(wv_hbm, wv, load_sem.at[2])

    def chunk_of(k):
        return k // per_micro, pl.ds(pl.multiple_of(lax.rem(k, per_micro) * CHUNK, CHUNK), CHUNK)

    def top_load(k):
        m, at_rows = chunk_of(k)
        return pltpu.make_async_copy(cot_hbm.at[m, at_rows], gb.at[m, at_rows], g_recv.at[k])

    def down(k):
        m, at_rows = chunk_of(k)
        return pltpu.make_async_remote_copy(
            src_ref=gout.at[m, at_rows],
            dst_ref=gb.at[m, at_rows],
            send_sem=g_send.at[k],
            recv_sem=g_recv.at[k],
            device_id=below,
            device_id_type=MESH,
        )

    def up(n):
        m, at_rows = chunk_of(downs + n)
        return pltpu.make_async_remote_copy(
            src_ref=gout.at[m, at_rows],
            dst_ref=ub.at[n],
            send_sem=g_send.at[downs + n],
            recv_sem=u_recv.at[n],
            device_id=up_far,
            device_id_type=MESH,
        )

    def onward(n):
        m, at_rows = chunk_of(downs + n)
        return pltpu.make_async_remote_copy(
            src_ref=ub.at[n],
            dst_ref=gb.at[m, at_rows],
            send_sem=u_send.at[n],
            recv_sem=g_recv.at[downs + n],
            device_id=up_far,
            device_id_type=MESH,
        )

    def relay(n):
        with jax.named_scope("relay"):
            up(n).wait_recv()
            onward(n).start()

    never = 4 * chunks
    relay_odd = jnp.where(sec == 0, -ups, jnp.where(sec == 2, 8, jnp.where(sec == 3, 7, never)))
    relay_even = jnp.where(sec == 0, 0, jnp.where(sec == 1, -1, jnp.where(sec == 3, 9, never)))
    relay_at = jnp.where(zi == 1, relay_odd, relay_even)
    lead = sections - sec

    def order(i):
        j = i - lead
        mixed = jnp.where(lax.rem(j, 2) == 0, downs + j // 2, lead + (j - 1) // 2)
        late = jnp.where(j < 2 * ups - 1, mixed, i - ups)
        return jnp.where(i < lead, i, late)

    is_top = sec == sections - 1
    wv_load.start()

    @pl.when(is_top)
    def _():
        @pl.loop(0, chunks)
        def _(k):
            top_load(k).start()

    wo_load.start()
    x_load.start()

    barrier = pltpu.get_barrier_semaphore()
    peers = [above, below, up_far, down_far, partner, z_peer] + x_peer[1:] + y_peer[1:]
    for peer in peers:
        pl.semaphore_signal(barrier, inc=1, device_id=peer, device_id_type=MESH)

    gain = gain_ref[...]

    def normed(x):
        inv = lax.rsqrt(jnp.mean(x * x, axis=-1, keepdims=True) + EPSILON)
        unit = x * inv
        return inv, unit, (unit * gain).astype(BF16)

    with jax.named_scope("loads"):
        gacc[...] = jnp.zeros_like(gacc)
        wv_load.wait()

        @pl.loop(0, width // 256)
        def _(b):
            at_cols = pl.ds(pl.multiple_of(b * 256, 256), 256)
            wvt[:, at_cols] = wv[at_cols, :].T

        wo_load.wait()
        x_load.wait()

    with jax.named_scope("barrier"):
        pl.semaphore_wait(barrier, len(peers))

    with jax.named_scope("prepare"):

        @pl.when(jnp.logical_not(is_top))
        def _():
            @pl.loop(0, micro)
            def _(m):
                slot = slot_ref[0, m]

                @pl.loop(0, per_micro)
                def _(j):
                    at_rows = pl.ds(pl.multiple_of(j * CHUNK, CHUNK), CHUNK)
                    _, _, n = normed(xb[slot, at_rows, :].astype(F32))
                    nb[m, at_rows, :] = n

                vb[m] = jnp.dot(nb[m], wv[...], preferred_element_type=F32).astype(BF16)

    def left_copy(k):
        m, at_rows = chunk_of(k)
        far = pl.ds(pl.multiple_of(tokens + lax.rem(k, per_micro) * CHUNK, CHUNK), CHUNK)
        return pltpu.make_async_remote_copy(
            src_ref=lo.at[m, at_rows],
            dst_ref=ll.at[m, far],
            send_sem=l_send.at[k],
            recv_sem=l_recv.at[k],
            device_id=partner,
            device_id_type=MESH,
        )

    def right_copy(k):
        m, at_rows = chunk_of(k)
        far = pl.ds(pl.multiple_of(tokens + lax.rem(k, per_micro) * CHUNK, CHUNK), CHUNK)
        return pltpu.make_async_remote_copy(
            src_ref=ro.at[m, at_rows],
            dst_ref=rr.at[m, far],
            send_sem=rr_send.at[k],
            recv_sem=rr_recv.at[k],
            device_id=partner,
            device_id_type=MESH,
        )

    wide = 256

    def received(m):
        @pl.loop(0, per_micro)
        def _(j):
            left_copy(m * per_micro + j).wait_recv()
            right_copy(m * per_micro + j).wait_recv()

    def add_columns(m, at_cols, first):
        term = lax.dot_general(
            ll[m], rr[m, :, at_cols], (((0,), (0,)), ((), ())), preferred_element_type=F32
        )
        if first:
            acc[:, at_cols] = term
        else:
            acc[:, at_cols] += term

    def accumulate(m, first):
        received(m)

        @pl.loop(0, inner // wide)
        def _(c):
            add_columns(m, pl.ds(pl.multiple_of(c * wide, wide), wide), first)

    @pl.loop(0, ups)
    def _(n):
        @pl.when(n < -relay_at)
        def _():
            relay(n)

    @pl.loop(0, chunks)
    def _(i):
        k = order(i)
        m, at_rows = chunk_of(k)
        pm, p_rows = chunk_of(i)

        with jax.named_scope("gwait"):

            @pl.when(is_top)
            def _():
                top_load(k).wait()

            @pl.when(jnp.logical_not(is_top))
            def _():
                down(k).wait_recv()

        with jax.named_scope("main"):
            g = gb[m, at_rows, :]
            inv, unit, n = normed(xb[slot_ref[0, m], at_rows, :].astype(F32))
            gv = jnp.dot(g, wo[...], preferred_element_type=F32).astype(BF16)
            gn = jnp.dot(gv, wvt[...], preferred_element_type=F32)
            gu_terms = gn * unit
            gu = gn * gain
            centre = jnp.mean(gu * unit, axis=-1, keepdims=True)
            gout[m, at_rows, :] = (g.astype(F32) + inv * (gu - unit * centre)).astype(BF16)
            part = gu_terms[0:8]
            for j in range(1, CHUNK // 8):
                part = part + gu_terms[8 * j : 8 * j + 8]
            gacc[...] += part

        with jax.named_scope("turn"):

            @pl.when(jnp.logical_and(is_top, jnp.logical_and(k > 0, k < downs)))
            def _():
                @pl.when(zi == 0)
                def _():
                    down(k - 1).wait_send()
                    pl.semaphore_signal(turn, inc=1, device_id=z_peer, device_id_type=MESH)

                @pl.when(zi == 1)
                def _():
                    pl.semaphore_wait(turn, 1)

        @pl.when(jnp.logical_and(sec > 0, k < downs))
        def _():
            down(k).start()

        @pl.when(jnp.logical_and(sec > 0, k >= downs))
        def _():
            up(k - downs).start()

        with jax.named_scope("share"):

            @pl.when(is_top)
            def _():
                vb[m, at_rows, :] = jnp.dot(n, wv[...], preferred_element_type=F32).astype(BF16)

            v = vb[m, at_rows, :]
            ll[pm, p_rows, :] = jnp.where(core == 0, n, g)
            lo[pm, p_rows, :] = jnp.where(core == 0, g, n)
            rr[pm, p_rows, :] = jnp.where(core == 0, gv, v)
            ro[pm, p_rows, :] = jnp.where(core == 0, v, gv)
            left_copy(i).start()
            right_copy(i).start()

        @pl.when(jnp.logical_and(i >= relay_at, i < relay_at + ups))
        def _():
            relay(i - relay_at)

        @pl.when(i == per_micro + 1)
        def _():
            with jax.named_scope("acc"):
                accumulate(0, True)

        if micro > 2:

            @pl.when(jnp.logical_and(lax.rem(i, per_micro) == 1, i > 2 * per_micro))
            def _():
                with jax.named_scope("acc"):
                    accumulate(pm - 1, False)

    own_gain = jnp.sum(gacc[...], axis=0, keepdims=True)
    gc[core] = own_gain
    gc_copy = pltpu.make_async_remote_copy(
        src_ref=gc.at[core],
        dst_ref=gc.at[core],
        send_sem=gc_send,
        recv_sem=gc_recv,
        device_id=partner,
        device_id_type=MESH,
    )
    gc_copy.start()

    received(micro - 1)

    def pieces(y, z, x):
        p = (y * NZ + z) * NX + x
        return pl.ds(pl.multiple_of(p * rows, 8), rows)

    def group(block_rows, g):
        lane = g * LANES
        top = acc[block_rows, lane : lane + LANES]
        bottom = acc[block_rows, inner // 2 + lane : inner // 2 + lane + LANES]
        return jnp.concatenate([top, bottom], axis=0)

    def stage_ring(part, dest, hs):
        @pl.loop(0, NY * NZ)
        def _(j):
            other, z = j // NZ, lax.rem(j, NZ)
            block_rows = pieces(other, z, dest) if part == 0 else pieces(dest, z, other)
            first_group = group(block_rows, 2 * part)
            if 0 in hs:
                st1[part, dest, 0, j] = first_group[:HALF_ROWS].astype(BF16)
            if 1 in hs:
                rest = group(block_rows, 2 * part + 1)[: 2 * HALF_ROWS - 2 * rows]
                st1[part, dest, 1, j] = jnp.concatenate(
                    [first_group[HALF_ROWS:], rest], axis=0
                ).astype(BF16)

    def stage_pair(part, dest):
        @pl.loop(0, NY * NX)
        def _(j):
            block_rows = pieces(j // NX, dest, lax.rem(j, NX))
            rest = group(block_rows, 2 * part + 1)[2 * rows - 2 * PAIR_ROWS :]
            stc[part, dest, j] = rest.astype(BF16)

    def ring_copy(st, r, send, recv, part, slot, src, h, peer):
        return pltpu.make_async_remote_copy(
            src_ref=st.at[part, src, h],
            dst_ref=r.at[part, slot],
            send_sem=send.at[part, slot],
            recv_sem=recv.at[part, slot],
            device_id=peer,
            device_id_type=MESH,
        )

    def neighbours(i, n):
        return lax.rem(i + 1, n), lax.rem(i + 3, n), lax.rem(i + 2, n)

    def ring(st, r, send, recv, part, mine, n, peer):
        plus, minus, across = neighbours(mine, n)
        to_plus, to_minus = peer[1], peer[3]
        copy = functools.partial(ring_copy, st, r, send, recv, part)
        return [
            copy(0, across, 0, to_plus),
            copy(1, across, 1, to_minus),
            copy(2, plus, 1, to_plus),
            copy(3, minus, 0, to_minus),
            copy(4, plus, 0, to_plus),
            copy(5, minus, 1, to_minus),
        ]

    def hop(st, r, copies, part, mine, n, loops):
        plus, minus, across = neighbours(mine, n)
        for slot, dest, h, forward in ((0, plus, 0, 4), (1, minus, 1, 5)):
            copies[slot].wait_recv()

            @pl.loop(0, loops)
            def _(j):
                st[part, dest, h, j] = (
                    st[part, dest, h, j].astype(F32) + r[part, slot, j].astype(F32)
                ).astype(BF16)

            copies[forward].start()

    def collect(st, r, copies, part, mine, loops, put):
        for h, slots in ((0, (3, 4)), (1, (2, 5))):
            for slot in slots:
                copies[slot].wait_recv()

            @pl.loop(0, loops)
            def _(j):
                put(
                    h,
                    j,
                    st[part, mine, h, j].astype(F32)
                    + r[part, slots[0], j].astype(F32)
                    + r[part, slots[1], j].astype(F32),
                )

    dims = [(xi, NX, x_peer), (yi, NY, y_peer)]
    first = [ring(st1, r1, s1_send, s1_recv, part, *dims[part]) for part in range(2)]
    second = [ring(st2, r2, s2_send, s2_recv, part, *dims[1 - part]) for part in range(2)]
    fourth = [ring(st4, r4, s4_send, s4_recv, part, *dims[part]) for part in range(2)]
    fifth = [ring(st5, r5, s5_send, s5_recv, part, *dims[1 - part]) for part in range(2)]

    def pair_copy(part):
        return pltpu.make_async_remote_copy(
            src_ref=stc.at[part, 1 - zi],
            dst_ref=rc.at[part],
            send_sem=sc_send.at[part],
            recv_sem=sc_recv.at[part],
            device_id=z_peer,
            device_id_type=MESH,
        )

    def z_copy(part):
        return pltpu.make_async_remote_copy(
            src_ref=st3.at[part, 1 - zi],
            dst_ref=r3.at[part],
            send_sem=s3_send.at[part],
            recv_sem=s3_recv.at[part],
            device_id=z_peer,
            device_id_type=MESH,
        )

    with jax.named_scope("stage"):
        for part in range(2):
            plus, minus, across = neighbours(*dims[part][:2])
            for side in range(2):
                lane = side * (inner // 2) + part * 2 * LANES
                add_columns(micro - 1, pl.ds(lane, wide), False)
            stage_ring(part, across, (0, 1))
            first[part][0].start()
            first[part][1].start()
            stage_pair(part, 1 - zi)
            pair_copy(part).start()

    gc_copy.wait_recv()
    gx[xi] = gc[0] + gc[1]
    gx_copies = []
    for d in range(1, NX):
        copy = pltpu.make_async_remote_copy(
            src_ref=gx.at[xi],
            dst_ref=gx.at[xi],
            send_sem=gx_send.at[d],
            recv_sem=gx_recv.at[xi],
            device_id=x_peer[d],
            device_id_type=MESH,
        )
        copy.start()
        gx_copies.append(copy)

    with jax.named_scope("stage2"):
        for part in range(2):
            plus, minus, across = neighbours(*dims[part][:2])
            stage_ring(part, plus, (0, 1))
            stage_ring(part, minus, (0, 1))
        for part in range(2):
            for j in range(2):
                first[part][j].wait_send()
                first[part][2 + j].start()
        for part in range(2):
            stage_ring(part, dims[part][0], (0, 1))
            stage_pair(part, zi)

    paced = jnp.logical_and(is_top, zi == 0)

    @pl.when(jnp.logical_and(sec > 0, jnp.logical_not(paced)))
    def _():
        @pl.loop(0, downs - 1)
        def _(k):
            down(k).wait_send()

    @pl.when(sec > 0)
    def _():
        down(downs - 1).wait_send()

        @pl.loop(0, ups)
        def _(n):
            up(n).wait_send()

    @pl.when(relay_at < never)
    def _():
        @pl.loop(0, ups)
        def _(n):
            onward(n).wait_send()

    @pl.loop(0, chunks)
    def _(k):
        left_copy(k).wait_send()
        right_copy(k).wait_send()

    with jax.named_scope("hop1"):
        for part in range(2):
            hop(st1, r1, first[part], part, *dims[part][:2], NY * NZ)

    def gathered(buf, recv, mine, n):
        for d in range(1, n):
            j = lax.rem(mine + d, n)
            pltpu.make_async_remote_copy(
                src_ref=buf.at[j],
                dst_ref=buf.at[j],
                send_sem=gx_send.at[0],
                recv_sem=recv.at[j],
                device_id=partner,
                device_id_type=MESH,
            ).wait_recv()
        total = buf[0]
        for j in range(1, n):
            total = total + buf[j]
        return total

    gy[yi] = gathered(gx, gx_recv, xi, NX)
    gy_copies = []
    for d in range(1, NY):
        copy = pltpu.make_async_remote_copy(
            src_ref=gy.at[yi],
            dst_ref=gy.at[yi],
            send_sem=gy_send.at[d],
            recv_sem=gy_recv.at[yi],
            device_id=y_peer[d],
            device_id_type=MESH,
        )
        copy.start()
        gy_copies.append(copy)

    with jax.named_scope("pair"):
        for part in range(2):
            pair_copy(part).wait_recv()

            @pl.loop(0, NY * NX)
            def _(j):
                total = (stc[part, zi, j].astype(F32) + rc[part, j].astype(F32)).astype(BF16)
                y, x = j // NX, lax.rem(j, NX)
                dest, other = (x, y) if part == 0 else (y, x)
                st4[part, dest, 0, other] = total[: PAIR_ROWS]
                st4[part, dest, 1, other] = total[PAIR_ROWS:]

            for j in range(4):
                fourth[part][j].start()

    with jax.named_scope("sum1"):
        for part in range(2):

            def put(h, j, total):
                st2[part, j // NZ, h, lax.rem(j, NZ)] = total.astype(BF16)

            collect(st1, r1, first[part], part, dims[part][0], NY * NZ, put)
            for j in range(4):
                second[part][j].start()

    gz[zi] = gathered(gy, gy_recv, yi, NY)
    gz_copy = pltpu.make_async_remote_copy(
        src_ref=gz.at[zi],
        dst_ref=gz.at[zi],
        send_sem=gz_send,
        recv_sem=gz_recv,
        device_id=z_peer,
        device_id_type=MESH,
    )
    gz_copy.start()

    with jax.named_scope("hop4"):
        for part in range(2):
            hop(st4, r4, fourth[part], part, *dims[part][:2], NY)

    for part in range(2):
        for j in range(2, 6):
            first[part][j].wait_send()
        pair_copy(part).wait_send()

    with jax.named_scope("hop2"):
        for part in range(2):
            hop(st2, r2, second[part], part, *dims[1 - part][:2], NZ)

    with jax.named_scope("sum4"):
        for part in range(2):

            def put(h, j, total):
                st5[part, j, h, 0] = total.astype(BF16)

            collect(st4, r4, fourth[part], part, dims[part][0], NY, put)
            for j in range(4):
                fifth[part][j].start()

    with jax.named_scope("sum2"):
        for part in range(2):

            def put(h, j, total):
                st3[part, j, h] = total.astype(BF16)

            collect(st2, r2, second[part], part, dims[1 - part][0], NZ, put)
            z_copy(part).start()

    with jax.named_scope("hop5"):
        for part in range(2):
            hop(st5, r5, fifth[part], part, *dims[1 - part][:2], 1)

    for part in range(2):
        for j in range(6):
            second[part][j].wait_send()
            fourth[part][j].wait_send()
    for copy in [gc_copy] + gx_copies + gy_copies:
        copy.wait_send()

    def put_group(g, values):
        lane = g * LANES
        fin[:, lane : lane + LANES] = values[:rows]
        fin[:, inner // 2 + lane : inner // 2 + lane + LANES] = values[rows:]

    with jax.named_scope("sum5"):
        for part in range(2):
            mine = dims[1 - part][0]
            tail = []
            for h, slots in ((0, (3, 4)), (1, (2, 5))):
                for slot in slots:
                    fifth[part][slot].wait_recv()
                tail.append(
                    st5[part, mine, h, 0].astype(F32)
                    + r5[part, slots[0], 0].astype(F32)
                    + r5[part, slots[1], 0].astype(F32)
                )
            z_copy(part).wait_recv()
            a0 = st3[part, zi, 0].astype(F32) + r3[part, 0].astype(F32)
            a1 = st3[part, zi, 1].astype(F32) + r3[part, 1].astype(F32)
            rest = 2 * rows - HALF_ROWS
            put_group(2 * part, jnp.concatenate([a0, a1[:rest]], axis=0))
            put_group(2 * part + 1, jnp.concatenate([a1[rest:]] + tail, axis=0))

    with jax.named_scope("swap"):
        low, high = fin[0:half, :], fin[half:rows, :]
        give[...] = jnp.where(core == 0, high, low)
        swap = pltpu.make_async_remote_copy(
            src_ref=give,
            dst_ref=take,
            send_sem=f_send,
            recv_sem=f_recv,
            device_id=partner,
            device_id_type=MESH,
        )
        swap.start()
        keep = jnp.where(core == 0, low, high)
        gz_copy.wait_recv()
        og_ref[...] = gz[0] + gz[1]
        swap.wait_recv()
        other = take[...]
        ov_ref[...] = jnp.where(core == 0, keep, other)
        oo_ref[...] = jnp.where(core == 0, other, keep)

    with jax.named_scope("drain2"):
        for part in range(2):
            for j in range(6):
                fifth[part][j].wait_send()
            z_copy(part).wait_send()
        for copy in [gz_copy, swap]:
            copy.wait_send()


def hand_out(ov, oo, og, ov_out, oo_out, og_out):
    ov_out[:, 0, :] = ov[...]
    oo_out[:, 0, :] = oo[...]
    og_out[...] = og[...]


def per_device(sections, saved, cotangent, slot_table, gain, value_weight, out_weight):
    micro, tokens, width = cotangent.shape
    inner = value_weight.shape[2]
    rows = width // (NY * NZ * NX)
    chunks = micro * (tokens // CHUNK)
    long, short = (HALF_ROWS, LANES), (PAIR_ROWS, LANES)
    n1 = NY * NZ
    dma = pltpu.SemaphoreType.DMA
    hbm = pl.BlockSpec(memory_space=pl.ANY)
    vmem = pl.BlockSpec(memory_space=pltpu.VMEM)
    ov, oo, og = pl.pallas_call(
        functools.partial(kernel, sections),
        out_shape=(
            jax.ShapeDtypeStruct((rows // NC, inner), F32),
            jax.ShapeDtypeStruct((rows // NC, inner), F32),
            jax.ShapeDtypeStruct((1, width), F32),
        ),
        in_specs=[pl.BlockSpec(memory_space=pltpu.SMEM), vmem, hbm, hbm, hbm, hbm],
        out_specs=(vmem, vmem, vmem),
        scratch_shapes=[
            pltpu.VMEM((micro, tokens, width), BF16),
            pltpu.VMEM((micro, tokens, width), BF16),
            pltpu.VMEM((width, inner), BF16),
            pltpu.VMEM((width, inner), BF16),
            pltpu.VMEM((inner, width), BF16),
            pltpu.VMEM((micro, tokens, width), BF16),
            pltpu.VMEM((micro, tokens, inner), BF16),
            pltpu.VMEM((micro, tokens, width), BF16),
            pltpu.VMEM((micro, 2 * tokens, width), BF16),
            pltpu.VMEM((micro, 2 * tokens, inner), BF16),
            pltpu.VMEM((micro, tokens, width), BF16),
            pltpu.VMEM((micro, tokens, inner), BF16),
            pltpu.VMEM((width, inner), F32),
            pltpu.VMEM((8, width), F32),
            pltpu.VMEM((2, 4, 2, n1) + long, BF16),
            pltpu.VMEM((2, 6, n1) + long, BF16),
            pltpu.VMEM((2, 4, 2, NZ) + long, BF16),
            pltpu.VMEM((2, 6, NZ) + long, BF16),
            pltpu.VMEM((2, NZ, 2) + long, BF16),
            pltpu.VMEM((2, 2) + long, BF16),
            pltpu.VMEM((2, NZ, NY * NX, 2 * PAIR_ROWS, LANES), BF16),
            pltpu.VMEM((2, NY * NX, 2 * PAIR_ROWS, LANES), BF16),
            pltpu.VMEM((2, 4, 2, 4) + short, BF16),
            pltpu.VMEM((2, 6, 4) + short, BF16),
            pltpu.VMEM((2, 4, 2, 1) + short, BF16),
            pltpu.VMEM((2, 6, 1) + short, BF16),
            pltpu.VMEM((rows, inner), F32),
            pltpu.VMEM((rows // NC, inner), F32),
            pltpu.VMEM((rows // NC, inner), F32),
            pltpu.VMEM((NC, 1, width), F32),
            pltpu.VMEM((NX, 1, width), F32),
            pltpu.VMEM((NY, 1, width), F32),
            pltpu.VMEM((NZ, 1, width), F32),
            dma((3,)),
            dma((chunks,)),
            dma((chunks,)),
            dma((chunks,)),
            dma((chunks,)),
            dma((chunks,)),
            dma((chunks,)),
            dma((2, 6)),
            dma((2, 6)),
            dma((2, 6)),
            dma((2, 6)),
            dma((2,)),
            dma((2,)),
            dma((2,)),
            dma((2,)),
            dma((2, 6)),
            dma((2, 6)),
            dma((2, 6)),
            dma((2, 6)),
            dma,
            dma,
            dma,
            dma,
            dma((NX,)),
            dma((NX,)),
            dma((NY,)),
            dma((NY,)),
            dma,
            dma,
            pltpu.SemaphoreType.REGULAR,
            pltpu.VMEM((chunks // 4, CHUNK, width), BF16),
            dma((chunks // 4,)),
            dma((chunks // 4,)),
        ],
        compiler_params=pltpu.CompilerParams(
            collective_id=0, has_side_effects=True, vmem_limit_bytes=62 * 1024 * 1024
        ),
    )(slot_table, gain, saved[0], cotangent, value_weight[0], out_weight[0])
    ov, oo, og = pl.pallas_call(
        hand_out,
        out_shape=(
            jax.ShapeDtypeStruct((rows // NC, 1, inner), F32),
            jax.ShapeDtypeStruct((rows // NC, 1, inner), F32),
            jax.ShapeDtypeStruct((1, width), F32),
        ),
        in_specs=[vmem, vmem, vmem],
        out_specs=(vmem, vmem, vmem),
    )(ov, oo, og)
    return (jnp.transpose(ov, (1, 0, 2)), jnp.transpose(oo, (1, 0, 2)), og)


def solution(mesh):
    in_specs = (
        P("section", None, "seq", None),
        P(None, "seq", None),
        P("section", None),
        P("section", None),
        P("section", None, None),
        P("section", None, None),
    )
    out_specs = (P("section", "seq", None), P("section", "seq", None), P("section", None))
    return jax.shard_map(
        functools.partial(per_device, mesh.shape["section"]),
        mesh=mesh,
        in_specs=in_specs,
        out_specs=out_specs,
        check_vma=False,
    )
```

```python
import functools

import jax
import jax.numpy as jnp
from jax import lax
from jax.experimental import pallas as pl
from jax.experimental.pallas import tpu as pltpu
from jax.sharding import PartitionSpec as P

EPSILON = 1e-06
MESH = pl.DeviceIdType.MESH
F32 = jnp.float32
BF16 = jnp.bfloat16

CHUNK = 32
NY, NZ, NX, NC = 4, 2, 4, 2
LANES = 128
HALF_ROWS = 112
PAIR_ROWS = 32


def kernel(
    sections,
    slot_ref,
    gain_ref,
    x_hbm,
    cot_hbm,
    wv_hbm,
    wo_hbm,
    ov_ref,
    oo_ref,
    og_ref,
    xb,
    gb,
    wv,
    wo,
    wvt,
    nb,
    vb,
    gout,
    ll,
    rr,
    lo,
    ro,
    acc,
    gacc,
    st1,
    r1,
    st2,
    r2,
    st3,
    r3,
    stc,
    rc,
    st4,
    r4,
    st5,
    r5,
    fin,
    give,
    take,
    gc,
    gx,
    gy,
    gz,
    load_sem,
    g_send,
    g_recv,
    l_send,
    l_recv,
    rr_send,
    rr_recv,
    s1_send,
    s1_recv,
    s2_send,
    s2_recv,
    s3_send,
    s3_recv,
    sc_send,
    sc_recv,
    s4_send,
    s4_recv,
    s5_send,
    s5_recv,
    f_send,
    f_recv,
    gc_send,
    gc_recv,
    gx_send,
    gx_recv,
    gy_send,
    gy_recv,
    gz_send,
    gz_recv,
    turn,
    ub,
    u_recv,
    u_send,
):
    micro, tokens, width = xb.shape
    inner = wv.shape[1]
    per_micro = tokens // CHUNK
    chunks = micro * per_micro
    rows = width // (NY * NZ * NX)
    half = rows // NC
    ups = chunks // 4
    downs = chunks - ups

    sec = lax.axis_index("section")
    q = lax.axis_index("seq")
    core = lax.rem(q, NC)
    xi = lax.rem(q // NC, NX)
    zi = lax.rem(q // (NC * NX), NZ)
    yi = q // (NC * NX * NZ)

    def at(y, z, x, c):
        return (sec, ((y * NZ + z) * NX + x) * NC + c)

    partner = at(yi, zi, xi, 1 - core)
    x_peer = [at(yi, zi, lax.rem(xi + d, NX), core) for d in range(NX)]
    y_peer = [at(lax.rem(yi + d, NY), zi, xi, core) for d in range(NY)]
    z_peer = at(yi, 1 - zi, xi, core)
    above = (lax.rem(sec + 1, sections), q)
    below = (lax.rem(sec + sections - 1, sections), q)

    def along_z(steps):
        z = lax.rem(sec * NZ + zi + steps, sections * NZ)
        return (z // NZ, ((yi * NZ + lax.rem(z, NZ)) * NX + xi) * NC + core)

    up_far, down_far = along_z(3), along_z(sections * NZ - 3)

    wo_load = pltpu.make_async_copy(wo_hbm, wo, load_sem.at[0])
    x_load = pltpu.make_async_copy(x_hbm, xb, load_sem.at[1])
    wv_load = pltpu.make_async_copy(wv_hbm, wv, load_sem.at[2])

    def chunk_of(k):
        return k // per_micro, pl.ds(pl.multiple_of(lax.rem(k, per_micro) * CHUNK, CHUNK), CHUNK)

    def top_load(k):
        m, at_rows = chunk_of(k)
        return pltpu.make_async_copy(cot_hbm.at[m, at_rows], gb.at[m, at_rows], g_recv.at[k])

    def down(k):
        m, at_rows = chunk_of(k)
        return pltpu.make_async_remote_copy(
            src_ref=gout.at[m, at_rows],
            dst_ref=gb.at[m, at_rows],
            send_sem=g_send.at[k],
            recv_sem=g_recv.at[k],
            device_id=below,
            device_id_type=MESH,
        )

    def up(n):
        m, at_rows = chunk_of(downs + n)
        return pltpu.make_async_remote_copy(
            src_ref=gout.at[m, at_rows],
            dst_ref=ub.at[n],
            send_sem=g_send.at[downs + n],
            recv_sem=u_recv.at[n],
            device_id=up_far,
            device_id_type=MESH,
        )

    def onward(n):
        m, at_rows = chunk_of(downs + n)
        return pltpu.make_async_remote_copy(
            src_ref=ub.at[n],
            dst_ref=gb.at[m, at_rows],
            send_sem=u_send.at[n],
            recv_sem=g_recv.at[downs + n],
            device_id=up_far,
            device_id_type=MESH,
        )

    def relay(n):
        with jax.named_scope("relay"):
            up(n).wait_recv()
            onward(n).start()

    never = 4 * chunks
    relay_odd = jnp.where(sec == 0, -ups, jnp.where(sec == 2, 8, jnp.where(sec == 3, 7, never)))
    relay_even = jnp.where(sec == 0, 0, jnp.where(sec == 1, -2, jnp.where(sec == 3, 9, never)))
    relay_at = jnp.where(zi == 1, relay_odd, relay_even)
    lead = sections - sec

    def order(i):
        j = i - lead
        mixed = jnp.where(lax.rem(j, 2) == 0, downs + j // 2, lead + (j - 1) // 2)
        late = jnp.where(j < 2 * ups - 1, mixed, i - ups)
        return jnp.where(i < lead, i, late)

    is_top = sec == sections - 1
    wv_load.start()

    @pl.when(is_top)
    def _():
        @pl.loop(0, chunks)
        def _(k):
            top_load(k).start()

    wo_load.start()
    x_load.start()

    barrier = pltpu.get_barrier_semaphore()
    peers = [above, below, up_far, down_far, partner, z_peer] + x_peer[1:] + y_peer[1:]
    for peer in peers:
        pl.semaphore_signal(barrier, inc=1, device_id=peer, device_id_type=MESH)

    gain = gain_ref[...]

    def normed(x):
        inv = lax.rsqrt(jnp.mean(x * x, axis=-1, keepdims=True) + EPSILON)
        unit = x * inv
        return inv, unit, (unit * gain).astype(BF16)

    with jax.named_scope("loads"):
        gacc[...] = jnp.zeros_like(gacc)
        wv_load.wait()

        @pl.loop(0, width // 256)
        def _(b):
            at_cols = pl.ds(pl.multiple_of(b * 256, 256), 256)
            wvt[:, at_cols] = wv[at_cols, :].T

        wo_load.wait()
        x_load.wait()

    with jax.named_scope("barrier"):
        pl.semaphore_wait(barrier, len(peers))

    with jax.named_scope("prepare"):

        @pl.when(jnp.logical_not(is_top))
        def _():
            @pl.loop(0, micro)
            def _(m):
                slot = slot_ref[0, m]

                @pl.loop(0, per_micro)
                def _(j):
                    at_rows = pl.ds(pl.multiple_of(j * CHUNK, CHUNK), CHUNK)
                    _, _, n = normed(xb[slot, at_rows, :].astype(F32))
                    nb[m, at_rows, :] = n

                vb[m] = jnp.dot(nb[m], wv[...], preferred_element_type=F32).astype(BF16)

    def left_copy(k):
        m, at_rows = chunk_of(k)
        far = pl.ds(pl.multiple_of(tokens + lax.rem(k, per_micro) * CHUNK, CHUNK), CHUNK)
        return pltpu.make_async_remote_copy(
            src_ref=lo.at[m, at_rows],
            dst_ref=ll.at[m, far],
            send_sem=l_send.at[k],
            recv_sem=l_recv.at[k],
            device_id=partner,
            device_id_type=MESH,
        )

    def right_copy(k):
        m, at_rows = chunk_of(k)
        far = pl.ds(pl.multiple_of(tokens + lax.rem(k, per_micro) * CHUNK, CHUNK), CHUNK)
        return pltpu.make_async_remote_copy(
            src_ref=ro.at[m, at_rows],
            dst_ref=rr.at[m, far],
            send_sem=rr_send.at[k],
            recv_sem=rr_recv.at[k],
            device_id=partner,
            device_id_type=MESH,
        )

    wide = 256

    def received(m):
        @pl.loop(0, per_micro)
        def _(j):
            left_copy(m * per_micro + j).wait_recv()
            right_copy(m * per_micro + j).wait_recv()

    def add_columns(m, at_cols, first):
        term = lax.dot_general(
            ll[m], rr[m, :, at_cols], (((0,), (0,)), ((), ())), preferred_element_type=F32
        )
        if first:
            acc[:, at_cols] = term
        else:
            acc[:, at_cols] += term

    def accumulate(m, first):
        received(m)

        @pl.loop(0, inner // wide)
        def _(c):
            add_columns(m, pl.ds(pl.multiple_of(c * wide, wide), wide), first)

    @pl.loop(0, ups)
    def _(n):
        @pl.when(n < -relay_at)
        def _():
            relay(n)

    @pl.loop(0, chunks)
    def _(i):
        k = order(i)
        m, at_rows = chunk_of(k)
        pm, p_rows = chunk_of(i)

        with jax.named_scope("gwait"):

            @pl.when(is_top)
            def _():
                top_load(k).wait()

            @pl.when(jnp.logical_not(is_top))
            def _():
                down(k).wait_recv()

        with jax.named_scope("main"):
            g = gb[m, at_rows, :]
            inv, unit, n = normed(xb[slot_ref[0, m], at_rows, :].astype(F32))
            gv = jnp.dot(g, wo[...], preferred_element_type=F32).astype(BF16)
            gn = jnp.dot(gv, wvt[...], preferred_element_type=F32)
            gu_terms = gn * unit
            gu = gn * gain
            centre = jnp.mean(gu * unit, axis=-1, keepdims=True)
            gout[m, at_rows, :] = (g.astype(F32) + inv * (gu - unit * centre)).astype(BF16)
            part = gu_terms[0:8]
            for j in range(1, CHUNK // 8):
                part = part + gu_terms[8 * j : 8 * j + 8]
            gacc[...] += part

        with jax.named_scope("turn"):

            @pl.when(jnp.logical_and(is_top, jnp.logical_and(k > 0, k < downs)))
            def _():
                @pl.when(zi == 0)
                def _():
                    down(k - 1).wait_send()
                    pl.semaphore_signal(turn, inc=1, device_id=z_peer, device_id_type=MESH)

                @pl.when(zi == 1)
                def _():
                    pl.semaphore_wait(turn, 1)

        @pl.when(jnp.logical_and(sec > 0, k < downs))
        def _():
            down(k).start()

        @pl.when(jnp.logical_and(sec > 0, k >= downs))
        def _():
            up(k - downs).start()

        with jax.named_scope("share"):

            @pl.when(is_top)
            def _():
                vb[m, at_rows, :] = jnp.dot(n, wv[...], preferred_element_type=F32).astype(BF16)

            v = vb[m, at_rows, :]
            ll[pm, p_rows, :] = jnp.where(core == 0, n, g)
            lo[pm, p_rows, :] = jnp.where(core == 0, g, n)
            rr[pm, p_rows, :] = jnp.where(core == 0, gv, v)
            ro[pm, p_rows, :] = jnp.where(core == 0, v, gv)
            left_copy(i).start()
            right_copy(i).start()

        @pl.when(jnp.logical_and(i >= relay_at, i < relay_at + ups))
        def _():
            relay(i - relay_at)

        @pl.when(i == per_micro + 1)
        def _():
            with jax.named_scope("acc"):
                accumulate(0, True)

        if micro > 2:

            @pl.when(jnp.logical_and(lax.rem(i, per_micro) == 1, i > 2 * per_micro))
            def _():
                with jax.named_scope("acc"):
                    accumulate(pm - 1, False)

    own_gain = jnp.sum(gacc[...], axis=0, keepdims=True)
    gc[core] = own_gain
    gc_copy = pltpu.make_async_remote_copy(
        src_ref=gc.at[core],
        dst_ref=gc.at[core],
        send_sem=gc_send,
        recv_sem=gc_recv,
        device_id=partner,
        device_id_type=MESH,
    )
    gc_copy.start()

    received(micro - 1)

    def pieces(y, z, x):
        p = (y * NZ + z) * NX + x
        return pl.ds(pl.multiple_of(p * rows, 8), rows)

    def group(block_rows, g):
        lane = g * LANES
        top = acc[block_rows, lane : lane + LANES]
        bottom = acc[block_rows, inner // 2 + lane : inner // 2 + lane + LANES]
        return jnp.concatenate([top, bottom], axis=0)

    def stage_ring(part, dest, hs):
        @pl.loop(0, NY * NZ)
        def _(j):
            other, z = j // NZ, lax.rem(j, NZ)
            block_rows = pieces(other, z, dest) if part == 0 else pieces(dest, z, other)
            first_group = group(block_rows, 2 * part)
            if 0 in hs:
                st1[part, dest, 0, j] = first_group[:HALF_ROWS].astype(BF16)
            if 1 in hs:
                rest = group(block_rows, 2 * part + 1)[: 2 * HALF_ROWS - 2 * rows]
                st1[part, dest, 1, j] = jnp.concatenate(
                    [first_group[HALF_ROWS:], rest], axis=0
                ).astype(BF16)

    def stage_pair(part, dest):
        @pl.loop(0, NY * NX)
        def _(j):
            block_rows = pieces(j // NX, dest, lax.rem(j, NX))
            rest = group(block_rows, 2 * part + 1)[2 * rows - 2 * PAIR_ROWS :]
            stc[part, dest, j] = rest.astype(BF16)

    def ring_copy(st, r, send, recv, part, slot, src, h, peer):
        return pltpu.make_async_remote_copy(
            src_ref=st.at[part, src, h],
            dst_ref=r.at[part, slot],
            send_sem=send.at[part, slot],
            recv_sem=recv.at[part, slot],
            device_id=peer,
            device_id_type=MESH,
        )

    def neighbours(i, n):
        return lax.rem(i + 1, n), lax.rem(i + 3, n), lax.rem(i + 2, n)

    def ring(st, r, send, recv, part, mine, n, peer):
        plus, minus, across = neighbours(mine, n)
        to_plus, to_minus = peer[1], peer[3]
        copy = functools.partial(ring_copy, st, r, send, recv, part)
        return [
            copy(0, across, 0, to_plus),
            copy(1, across, 1, to_minus),
            copy(2, plus, 1, to_plus),
            copy(3, minus, 0, to_minus),
            copy(4, plus, 0, to_plus),
            copy(5, minus, 1, to_minus),
        ]

    def hop(st, r, copies, part, mine, n, loops):
        plus, minus, across = neighbours(mine, n)
        for slot, dest, h, forward in ((0, plus, 0, 4), (1, minus, 1, 5)):
            copies[slot].wait_recv()

            @pl.loop(0, loops)
            def _(j):
                st[part, dest, h, j] = (
                    st[part, dest, h, j].astype(F32) + r[part, slot, j].astype(F32)
                ).astype(BF16)

            copies[forward].start()

    def collect(st, r, copies, part, mine, loops, put):
        for h, slots in ((0, (3, 4)), (1, (2, 5))):
            for slot in slots:
                copies[slot].wait_recv()

            @pl.loop(0, loops)
            def _(j):
                put(
                    h,
                    j,
                    st[part, mine, h, j].astype(F32)
                    + r[part, slots[0], j].astype(F32)
                    + r[part, slots[1], j].astype(F32),
                )

    dims = [(xi, NX, x_peer), (yi, NY, y_peer)]
    first = [ring(st1, r1, s1_send, s1_recv, part, *dims[part]) for part in range(2)]
    second = [ring(st2, r2, s2_send, s2_recv, part, *dims[1 - part]) for part in range(2)]
    fourth = [ring(st4, r4, s4_send, s4_recv, part, *dims[part]) for part in range(2)]
    fifth = [ring(st5, r5, s5_send, s5_recv, part, *dims[1 - part]) for part in range(2)]

    def pair_copy(part):
        return pltpu.make_async_remote_copy(
            src_ref=stc.at[part, 1 - zi],
            dst_ref=rc.at[part],
            send_sem=sc_send.at[part],
            recv_sem=sc_recv.at[part],
            device_id=z_peer,
            device_id_type=MESH,
        )

    def z_copy(part):
        return pltpu.make_async_remote_copy(
            src_ref=st3.at[part, 1 - zi],
            dst_ref=r3.at[part],
            send_sem=s3_send.at[part],
            recv_sem=s3_recv.at[part],
            device_id=z_peer,
            device_id_type=MESH,
        )

    with jax.named_scope("stage"):
        for part in range(2):
            plus, minus, across = neighbours(*dims[part][:2])
            for side in range(2):
                lane = side * (inner // 2) + part * 2 * LANES
                add_columns(micro - 1, pl.ds(lane, wide), False)
            stage_ring(part, across, (0, 1))
            first[part][0].start()
            first[part][1].start()
            stage_pair(part, 1 - zi)
            pair_copy(part).start()

    gc_copy.wait_recv()
    gx[xi] = gc[0] + gc[1]
    gx_copies = []
    for d in range(1, NX):
        copy = pltpu.make_async_remote_copy(
            src_ref=gx.at[xi],
            dst_ref=gx.at[xi],
            send_sem=gx_send.at[d],
            recv_sem=gx_recv.at[xi],
            device_id=x_peer[d],
            device_id_type=MESH,
        )
        copy.start()
        gx_copies.append(copy)

    with jax.named_scope("stage2"):
        for part in range(2):
            plus, minus, across = neighbours(*dims[part][:2])
            stage_ring(part, plus, (0, 1))
            stage_ring(part, minus, (0, 1))
        for part in range(2):
            for j in range(2):
                first[part][j].wait_send()
                first[part][2 + j].start()
        for part in range(2):
            stage_ring(part, dims[part][0], (0, 1))
            stage_pair(part, zi)

    paced = jnp.logical_and(is_top, zi == 0)

    @pl.when(jnp.logical_and(sec > 0, jnp.logical_not(paced)))
    def _():
        @pl.loop(0, downs - 1)
        def _(k):
            down(k).wait_send()

    @pl.when(sec > 0)
    def _():
        down(downs - 1).wait_send()

        @pl.loop(0, ups)
        def _(n):
            up(n).wait_send()

    @pl.when(relay_at < never)
    def _():
        @pl.loop(0, ups)
        def _(n):
            onward(n).wait_send()

    @pl.loop(0, chunks)
    def _(k):
        left_copy(k).wait_send()
        right_copy(k).wait_send()

    with jax.named_scope("hop1"):
        for part in range(2):
            hop(st1, r1, first[part], part, *dims[part][:2], NY * NZ)

    def gathered(buf, recv, mine, n):
        for d in range(1, n):
            j = lax.rem(mine + d, n)
            pltpu.make_async_remote_copy(
                src_ref=buf.at[j],
                dst_ref=buf.at[j],
                send_sem=gx_send.at[0],
                recv_sem=recv.at[j],
                device_id=partner,
                device_id_type=MESH,
            ).wait_recv()
        total = buf[0]
        for j in range(1, n):
            total = total + buf[j]
        return total

    gy[yi] = gathered(gx, gx_recv, xi, NX)
    gy_copies = []
    for d in range(1, NY):
        copy = pltpu.make_async_remote_copy(
            src_ref=gy.at[yi],
            dst_ref=gy.at[yi],
            send_sem=gy_send.at[d],
            recv_sem=gy_recv.at[yi],
            device_id=y_peer[d],
            device_id_type=MESH,
        )
        copy.start()
        gy_copies.append(copy)

    with jax.named_scope("pair"):
        for part in range(2):
            pair_copy(part).wait_recv()

            @pl.loop(0, NY * NX)
            def _(j):
                total = (stc[part, zi, j].astype(F32) + rc[part, j].astype(F32)).astype(BF16)
                y, x = j // NX, lax.rem(j, NX)
                dest, other = (x, y) if part == 0 else (y, x)
                st4[part, dest, 0, other] = total[: PAIR_ROWS]
                st4[part, dest, 1, other] = total[PAIR_ROWS:]

            for j in range(4):
                fourth[part][j].start()

    with jax.named_scope("sum1"):
        for part in range(2):

            def put(h, j, total):
                st2[part, j // NZ, h, lax.rem(j, NZ)] = total.astype(BF16)

            collect(st1, r1, first[part], part, dims[part][0], NY * NZ, put)
            for j in range(4):
                second[part][j].start()

    gz[zi] = gathered(gy, gy_recv, yi, NY)
    gz_copy = pltpu.make_async_remote_copy(
        src_ref=gz.at[zi],
        dst_ref=gz.at[zi],
        send_sem=gz_send,
        recv_sem=gz_recv,
        device_id=z_peer,
        device_id_type=MESH,
    )
    gz_copy.start()

    with jax.named_scope("hop4"):
        for part in range(2):
            hop(st4, r4, fourth[part], part, *dims[part][:2], NY)

    for part in range(2):
        for j in range(2, 6):
            first[part][j].wait_send()
        pair_copy(part).wait_send()

    with jax.named_scope("hop2"):
        for part in range(2):
            hop(st2, r2, second[part], part, *dims[1 - part][:2], NZ)

    with jax.named_scope("sum4"):
        for part in range(2):

            def put(h, j, total):
                st5[part, j, h, 0] = total.astype(BF16)

            collect(st4, r4, fourth[part], part, dims[part][0], NY, put)
            for j in range(4):
                fifth[part][j].start()

    with jax.named_scope("sum2"):
        for part in range(2):

            def put(h, j, total):
                st3[part, j, h] = total.astype(BF16)

            collect(st2, r2, second[part], part, dims[1 - part][0], NZ, put)
            z_copy(part).start()

    with jax.named_scope("hop5"):
        for part in range(2):
            hop(st5, r5, fifth[part], part, *dims[1 - part][:2], 1)

    for part in range(2):
        for j in range(6):
            second[part][j].wait_send()
            fourth[part][j].wait_send()
    for copy in [gc_copy] + gx_copies + gy_copies:
        copy.wait_send()

    def put_group(g, values):
        lane = g * LANES
        fin[:, lane : lane + LANES] = values[:rows]
        fin[:, inner // 2 + lane : inner // 2 + lane + LANES] = values[rows:]

    with jax.named_scope("sum5"):
        for part in range(2):
            mine = dims[1 - part][0]
            tail = []
            for h, slots in ((0, (3, 4)), (1, (2, 5))):
                for slot in slots:
                    fifth[part][slot].wait_recv()
                tail.append(
                    st5[part, mine, h, 0].astype(F32)
                    + r5[part, slots[0], 0].astype(F32)
                    + r5[part, slots[1], 0].astype(F32)
                )
            z_copy(part).wait_recv()
            a0 = st3[part, zi, 0].astype(F32) + r3[part, 0].astype(F32)
            a1 = st3[part, zi, 1].astype(F32) + r3[part, 1].astype(F32)
            rest = 2 * rows - HALF_ROWS
            put_group(2 * part, jnp.concatenate([a0, a1[:rest]], axis=0))
            put_group(2 * part + 1, jnp.concatenate([a1[rest:]] + tail, axis=0))

    with jax.named_scope("swap"):
        low, high = fin[0:half, :], fin[half:rows, :]
        give[...] = jnp.where(core == 0, high, low)
        swap = pltpu.make_async_remote_copy(
            src_ref=give,
            dst_ref=take,
            send_sem=f_send,
            recv_sem=f_recv,
            device_id=partner,
            device_id_type=MESH,
        )
        swap.start()
        keep = jnp.where(core == 0, low, high)
        gz_copy.wait_recv()
        og_ref[...] = gz[0] + gz[1]
        swap.wait_recv()
        other = take[...]
        ov_ref[...] = jnp.where(core == 0, keep, other)
        oo_ref[...] = jnp.where(core == 0, other, keep)

    with jax.named_scope("drain2"):
        for part in range(2):
            for j in range(6):
                fifth[part][j].wait_send()
            z_copy(part).wait_send()
        for copy in [gz_copy, swap]:
            copy.wait_send()


def hand_out(ov, oo, og, ov_out, oo_out, og_out):
    ov_out[:, 0, :] = ov[...]
    oo_out[:, 0, :] = oo[...]
    og_out[...] = og[...]


def per_device(sections, saved, cotangent, slot_table, gain, value_weight, out_weight):
    micro, tokens, width = cotangent.shape
    inner = value_weight.shape[2]
    rows = width // (NY * NZ * NX)
    chunks = micro * (tokens // CHUNK)
    long, short = (HALF_ROWS, LANES), (PAIR_ROWS, LANES)
    n1 = NY * NZ
    dma = pltpu.SemaphoreType.DMA
    hbm = pl.BlockSpec(memory_space=pl.ANY)
    vmem = pl.BlockSpec(memory_space=pltpu.VMEM)
    ov, oo, og = pl.pallas_call(
        functools.partial(kernel, sections),
        out_shape=(
            jax.ShapeDtypeStruct((rows // NC, inner), F32),
            jax.ShapeDtypeStruct((rows // NC, inner), F32),
            jax.ShapeDtypeStruct((1, width), F32),
        ),
        in_specs=[pl.BlockSpec(memory_space=pltpu.SMEM), vmem, hbm, hbm, hbm, hbm],
        out_specs=(vmem, vmem, vmem),
        scratch_shapes=[
            pltpu.VMEM((micro, tokens, width), BF16),
            pltpu.VMEM((micro, tokens, width), BF16),
            pltpu.VMEM((width, inner), BF16),
            pltpu.VMEM((width, inner), BF16),
            pltpu.VMEM((inner, width), BF16),
            pltpu.VMEM((micro, tokens, width), BF16),
            pltpu.VMEM((micro, tokens, inner), BF16),
            pltpu.VMEM((micro, tokens, width), BF16),
            pltpu.VMEM((micro, 2 * tokens, width), BF16),
            pltpu.VMEM((micro, 2 * tokens, inner), BF16),
            pltpu.VMEM((micro, tokens, width), BF16),
            pltpu.VMEM((micro, tokens, inner), BF16),
            pltpu.VMEM((width, inner), F32),
            pltpu.VMEM((8, width), F32),
            pltpu.VMEM((2, 4, 2, n1) + long, BF16),
            pltpu.VMEM((2, 6, n1) + long, BF16),
            pltpu.VMEM((2, 4, 2, NZ) + long, BF16),
            pltpu.VMEM((2, 6, NZ) + long, BF16),
            pltpu.VMEM((2, NZ, 2) + long, BF16),
            pltpu.VMEM((2, 2) + long, BF16),
            pltpu.VMEM((2, NZ, NY * NX, 2 * PAIR_ROWS, LANES), BF16),
            pltpu.VMEM((2, NY * NX, 2 * PAIR_ROWS, LANES), BF16),
            pltpu.VMEM((2, 4, 2, 4) + short, BF16),
            pltpu.VMEM((2, 6, 4) + short, BF16),
            pltpu.VMEM((2, 4, 2, 1) + short, BF16),
            pltpu.VMEM((2, 6, 1) + short, BF16),
            pltpu.VMEM((rows, inner), F32),
            pltpu.VMEM((rows // NC, inner), F32),
            pltpu.VMEM((rows // NC, inner), F32),
            pltpu.VMEM((NC, 1, width), F32),
            pltpu.VMEM((NX, 1, width), F32),
            pltpu.VMEM((NY, 1, width), F32),
            pltpu.VMEM((NZ, 1, width), F32),
            dma((3,)),
            dma((chunks,)),
            dma((chunks,)),
            dma((chunks,)),
            dma((chunks,)),
            dma((chunks,)),
            dma((chunks,)),
            dma((2, 6)),
            dma((2, 6)),
            dma((2, 6)),
            dma((2, 6)),
            dma((2,)),
            dma((2,)),
            dma((2,)),
            dma((2,)),
            dma((2, 6)),
            dma((2, 6)),
            dma((2, 6)),
            dma((2, 6)),
            dma,
            dma,
            dma,
            dma,
            dma((NX,)),
            dma((NX,)),
            dma((NY,)),
            dma((NY,)),
            dma,
            dma,
            pltpu.SemaphoreType.REGULAR,
            pltpu.VMEM((chunks // 4, CHUNK, width), BF16),
            dma((chunks // 4,)),
            dma((chunks // 4,)),
        ],
        compiler_params=pltpu.CompilerParams(
            collective_id=0, has_side_effects=True, vmem_limit_bytes=62 * 1024 * 1024
        ),
    )(slot_table, gain, saved[0], cotangent, value_weight[0], out_weight[0])
    ov, oo, og = pl.pallas_call(
        hand_out,
        out_shape=(
            jax.ShapeDtypeStruct((rows // NC, 1, inner), F32),
            jax.ShapeDtypeStruct((rows // NC, 1, inner), F32),
            jax.ShapeDtypeStruct((1, width), F32),
        ),
        in_specs=[vmem, vmem, vmem],
        out_specs=(vmem, vmem, vmem),
    )(ov, oo, og)
    return (jnp.transpose(ov, (1, 0, 2)), jnp.transpose(oo, (1, 0, 2)), og)


def solution(mesh):
    in_specs = (
        P("section", None, "seq", None),
        P(None, "seq", None),
        P("section", None),
        P("section", None),
        P("section", None, None),
        P("section", None, None),
    )
    out_specs = (P("section", "seq", None), P("section", "seq", None), P("section", None))
    return jax.shard_map(
        functools.partial(per_device, mesh.shape["section"]),
        mesh=mesh,
        in_specs=in_specs,
        out_specs=out_specs,
        check_vma=False,
    )
```
